16 devices in a mesh: dp: 2 (over y, z), tp: 8 (over x, core).
Axes of the slice: x: 4, y: 2, z: 1, core: 2. Of those that a mesh axis runs over, the one named last changes fastest.
The devices are a block of a 4x4x8 slice.
Arguments:
- x: bfloat16 [4096, 7168], P('dp'), parts along dimension 0
- gain: bfloat16 [7168], replicated
- wq: bfloat16 [7168, 7168], P(None, 'tp')
- wk: bfloat16 [7168, 7168], P(None, 'tp')
- wv: bfloat16 [7168, 7168], P(None, 'tp')
- wo: bfloat16 [7168, 7168], P('tp')
Outputs:
- output: bfloat16 [4096, 7168], P('dp'), parts along dimension 0
There are 2 independent parts. The reference program is written for one: setup_inputs(seed, part) draws one part's arguments, and reference() takes and returns one part's arrays. A program takes and returns all parts, laid end to end along the dimension named above; an argument that names none is the same for every part.
All inputs are finite; a program needn't handle non-finite values.
Results may differ from the reference program's by a relative error of at most 0.012.
Values are sent between devices in bfloat16 or wider.
A program may use at most 768 MiB of HBM per device.

```python
import jax
import jax.numpy as jnp
from jax import lax

ROWS = 2048
D = 7168
HEADS = 56
KV_HEADS = 56
HEAD = 128
THETA = 10000


def setup_inputs(seed: int = 0, part: int = 0) -> dict:
    kx, kn, kq, kk, kv, ko = jax.random.split(jax.random.key(seed), 6)

    def weights(key, rows, columns):
        return jax.random.normal(key, (rows, columns), jnp.float32) * rows**-0.5

    drawn = {
        "x": jax.random.normal(jax.random.fold_in(kx, part), (ROWS, D), jnp.float32),
        "gain": 1 + 0.1 * jax.random.normal(kn, (D,), jnp.float32),
        "wq": 2 * weights(kq, D, HEADS * HEAD),
        "wk": 2 * weights(kk, D, KV_HEADS * HEAD),
        "wv": 4 * weights(kv, D, KV_HEADS * HEAD),
        "wo": weights(ko, HEADS * HEAD, D),
    }
    return {k: v.astype(jnp.bfloat16) for k, v in drawn.items()}


def normed(x, gain):
    wide = x.astype(jnp.float32)
    scale = lax.rsqrt(jnp.mean(wide * wide, -1, keepdims=True) + 1e-6)
    return (wide * scale * gain.astype(jnp.float32)).astype(jnp.bfloat16)


def turned(t, place, theta):
    half = t.shape[-1] // 2
    angle = place.astype(jnp.float32)[:, None] * theta ** (-jnp.arange(half, dtype=jnp.float32) / half)
    cos, sin = jnp.cos(angle)[:, None], jnp.sin(angle)[:, None]
    a, b = t[..., :half].astype(jnp.float32), t[..., half:].astype(jnp.float32)
    return jnp.concatenate([a * cos - b * sin, b * cos + a * sin], -1).astype(jnp.bfloat16)


def matmul(a, w):
    return jnp.dot(a, w, preferred_element_type=jnp.float32).astype(jnp.bfloat16)


def einsum(form, a, b):
    return jnp.einsum(form, a.astype(jnp.float32), b.astype(jnp.float32))


def attention(q, k, v):
    scores = einsum("tgsd,ugd->gstu", q, k) * q.shape[-1] ** -0.5
    token = jnp.arange(q.shape[0])
    scores = jnp.where(token[:, None] >= token, scores, -jnp.inf)
    weights = jax.nn.softmax(scores, -1).astype(jnp.bfloat16)
    return einsum("gstu,ugd->tgsd", weights, v).astype(jnp.bfloat16)


def reference(x, gain, wq, wk, wv, wo):
    a, place = normed(x, gain), jnp.arange(ROWS)
    q = turned(matmul(a, wq).reshape(ROWS, HEADS, HEAD), place, THETA).reshape(ROWS, KV_HEADS, -1, HEAD)
    k = turned(matmul(a, wk).reshape(ROWS, KV_HEADS, HEAD), place, THETA)
    v = matmul(a, wv).reshape(ROWS, KV_HEADS, HEAD)
    seen = attention(q, k, v).reshape(ROWS, HEADS * HEAD)
    return (x.astype(jnp.float32) + jnp.dot(seen, wo, preferred_element_type=jnp.float32)).astype(jnp.bfloat16)
```

```python
import functools

import jax
import jax.numpy as jnp
import numpy as np
from jax import lax
from jax.experimental import pallas as pl
from jax.experimental.pallas import tpu as pltpu
from jax.sharding import PartitionSpec as P

HEAD = 128
THETA = 10000
ROWS = 256
SLOTS = 4
STRIP = 32
ONES = 16
NEG = -1e30
HIDDEN = 2 * NEG
LOG2E = 1.4426950408889634
OPP, LEFT, SELF, RIGHT = range(4)
TOWARDS = (RIGHT, LEFT)
FROM = (LEFT, RIGHT)
MESH = pl.DeviceIdType.MESH
F32, BF16 = jnp.float32, jnp.bfloat16


def _fit(size, want, unit=128):
    return max(n for n in range(unit, want + 1, unit) if size % n == 0)


def _dot(a, b, ca, cb):
    return lax.dot_general(a, b, (((ca,), (cb,)), ((), ())), preferred_element_type=F32)


def _kernel(
    group, x_hbm, gain_ref, wq_hbm, wk_hbm, wv_hbm, wo_hbm, cb_ref, sb_ref, ca_ref, sa_ref, y_hbm,
    x_s, a_s, w_s, acc_s, q_s, k_s, vt_s, top_s, mix_s, seen_s, own_s, swap_out, swap_in, rs1_out, rs1_in, rs2_out, rs2_in, fin_s, res_s,
    w_sem, x_sem, res_sem, swap_ss, swap_rs, rs1_ss, rs1_rs, rs2_ss, rs2_rs, ag1_ss, ag1_rs, ag2_ss, ag2_rs, pair_ss, pair_rs, put_sem,
):
    rows, depth = x_hbm.shape
    wide = wq_hbm.shape[1]
    piece = depth // group
    heads = wide // HEAD
    chunk = x_s.shape[0]
    chunks = rows // chunk
    half = chunk // 2
    blocks, _, kb = a_s.shape
    tiles = 3 * blocks + group
    e = HEAD**-0.5 * LOG2E

    me = lax.axis_index("tp")
    chips = group // 2
    chip, core = me // 2, me % 2
    places = [(chip + by) % chips for by in (2, chips - 1, 0, 1)]
    partner = {"tp": chip * 2 + 1 - core}
    beside = [{"tp": places[TOWARDS[d]] * 2 + core} for d in range(2)]

    def columns(place, whose):
        return pl.ds(pl.multiple_of((place * 2 + whose) * piece, piece), piece)

    def rows_of(c, part=None):
        if part is None:
            return pl.ds(pl.multiple_of(c * chunk, chunk), chunk)
        return pl.ds(pl.multiple_of(c * chunk + part * half, half), half)

    def part_rows(part):
        return pl.ds(part * half, half)

    def remote(src, dst, send, recv, to):
        return pltpu.make_async_remote_copy(src_ref=src, dst_ref=dst, send_sem=send, recv_sem=recv, device_id=to, device_id_type=MESH)

    def swap(c, j):
        return remote(swap_out.at[j], swap_in.at[c % 2, j], swap_ss.at[j], swap_rs.at[c % 2, j], partner)

    def rs1(c, d):
        return remote(rs1_out.at[d], rs1_in.at[c % 2, d], rs1_ss.at[d], rs1_rs.at[c % 2, d], beside[d])

    def rs2(c, d, part):
        return remote(
            rs2_out.at[d, part_rows(part)], rs2_in.at[c % 2, d, part_rows(part)], rs2_ss.at[d, part], rs2_rs.at[c % 2, d, part], beside[d]
        )

    def ag1(c, d, part):
        there = y_hbm.at[rows_of(c, part), columns(chip, core)]
        return remote(fin_s.at[part_rows(part)], there, ag1_ss.at[d, part], ag1_rs.at[c % 2, d, part], beside[d])

    def ag2(c, d):
        there = y_hbm.at[rows_of(c, d), columns(places[FROM[d]], core)]
        return remote(there, there, ag2_ss.at[d], ag2_rs.at[c % 2, d], beside[d])

    def pair(c, j):
        there = y_hbm.at[rows_of(c), columns(places[j], core)]
        return remote(fin_s if j == SELF else there, there, pair_ss.at[j], pair_rs.at[c % 2, j], partner)

    def put(c):
        return pltpu.make_async_copy(fin_s, y_hbm.at[rows_of(c), columns(chip, core)], put_sem)

    def residual(c):
        return pltpu.make_async_copy(x_hbm.at[rows_of(c), columns(chip, core)], res_s.at[c % 2], res_sem.at[c % 2])

    def load_x(c):
        return pltpu.make_async_copy(x_hbm.at[rows_of(c)], x_s, x_sem)

    def weight(ref, i, slot):
        return pltpu.make_async_copy(ref.at[pl.ds(pl.multiple_of(i * kb, kb), kb)], w_s.at[slot, pl.ds(0, kb), pl.ds(0, wide)], w_sem.at[slot])

    def out_weight(j, slot):
        place = (chip + 2 + j) % chips
        whose = jnp.where(j < chips, 1 - core, core)
        return pltpu.make_async_copy(wo_hbm.at[:, columns(place, whose)], w_s.at[slot, pl.ds(0, wide), pl.ds(0, piece)], w_sem.at[slot])

    def slot_of(c, t):
        return (c * tiles + t) % SLOTS

    def fetch(c, t):
        slot = slot_of(c, t)
        later = t >= tiles
        t = jnp.where(later, t - tiles, t)
        live = jnp.where(later, c + 1, c) < chunks
        for n, ref in enumerate((wq_hbm, wk_hbm, wv_hbm)):

            @pl.when(live & (t >= n * blocks) & (t < (n + 1) * blocks))
            def _():
                weight(ref, t - n * blocks, slot).start()

        @pl.when(live & (t >= 3 * blocks))
        def _():
            out_weight(t - 3 * blocks, slot).start()

    def strips(count, body):
        lax.fori_loop(0, count // STRIP, lambda r, _: body(pl.ds(pl.multiple_of(r * STRIP, STRIP), STRIP)), None)

    def strips_of(part, body):
        lax.fori_loop(
            0,
            half // STRIP,
            lambda r, _: body(pl.ds(pl.multiple_of(part * half + r * STRIP, STRIP), STRIP), pl.ds(pl.multiple_of(r * STRIP, STRIP), STRIP)),
            None,
        )

    def norm(c):
        load_x(c).wait()

        def body(r):
            total = jnp.zeros((STRIP, kb), F32)
            for i in range(blocks):
                part = x_s[r, i * kb : (i + 1) * kb].astype(F32)
                total += part * part
            scale = lax.rsqrt(jnp.sum(total, axis=-1, keepdims=True) / depth + 1e-6)
            for i in range(blocks):
                part = x_s[r, i * kb : (i + 1) * kb].astype(F32)
                a_s[i, r, :] = (part * scale * gain_ref[:, i * kb : (i + 1) * kb]).astype(BF16)

        strips(chunk, body)

        @pl.when(c + 1 < chunks)
        def _():
            load_x(c + 1).start()

    def project(c, n):
        def body(i, _):
            t = n * blocks + i
            slot = slot_of(c, t)
            weight((wq_hbm, wk_hbm, wv_hbm)[n], i, slot).wait()
            fetch(c, t + SLOTS - 1)
            product = _dot(a_s[i], w_s[slot, :kb, :wide], 1, 0)

            @pl.when(i == 0)
            def _():
                acc_s[...] = product

            @pl.when(i > 0)
            def _():
                acc_s[...] += product

        lax.fori_loop(0, blocks, body, None)

    def turn(c, ref, at):
        ca, sa = ca_ref[pl.ds(c, 1), :], sa_ref[pl.ds(c, 1), :]

        def body(r):
            cb, sb = cb_ref[r, :], sb_ref[r, :]
            cos, sin = ca * cb - sa * sb, sa * cb + ca * sb
            for h in range(heads):
                t = acc_s[r, h * HEAD : (h + 1) * HEAD].astype(BF16).astype(F32)
                turned = t * cos + pltpu.roll(t, HEAD // 2, 1) * sin
                ref[h, pl.ds(pl.multiple_of(at + r.start, STRIP), STRIP), :] = turned.astype(BF16)

        strips(chunk, body)

    def keep_values(c):
        for h in range(heads):
            vt_s[h, :HEAD, rows_of(c)] = acc_s[:, h * HEAD : (h + 1) * HEAD].astype(BF16).T

    def attend(c):
        top_s[...] = jnp.full(top_s.shape, NEG, F32)
        mix_s[...] = jnp.zeros(mix_s.shape, F32)

        def block(j, masked):
            here = rows_of(j)
            scores = [_dot(k_s[h, here, :], q_s[h], 1, 1) for h in range(heads)]
            if masked:
                ok = lax.broadcasted_iota(jnp.int32, (chunk, chunk), 1) >= lax.broadcasted_iota(jnp.int32, (chunk, chunk), 0)
            weights, keeps = [], []
            for h, s in enumerate(scores):
                if masked:
                    s = jnp.where(ok, s, HIDDEN)
                old = top_s[h : h + 1, :]
                top = jnp.maximum(old, s.max(axis=0, keepdims=True))
                top_s[h : h + 1, :] = top
                weights.append(jnp.exp2((s - top) * e).astype(BF16))
                keeps.append(jnp.exp2((old - top) * e))
            for h in range(heads):
                mix_s[h] = mix_s[h] * keeps[h] + _dot(vt_s[h, :, here], weights[h], 1, 0)

        lax.fori_loop(0, c, lambda j, _: block(j, False), None)
        block(c, True)
        for h in range(heads):
            out = mix_s[h, :HEAD, :] * (1 / mix_s[h, HEAD : HEAD + 1, :])
            seen_s[:, h * HEAD : (h + 1) * HEAD] = out.T.astype(BF16)

    def project_out(c):
        def body(j, _):
            t = 3 * blocks + j
            slot = slot_of(c, t)
            out_weight(j, slot).wait()
            fetch(c, t + SLOTS - 1)
            product = _dot(seen_s[...], w_s[slot, :wide, :piece], 1, 0)

            @pl.when(j < chips)
            def _():
                @pl.when(c > 0)
                def _():
                    swap(c - 1, j).wait_send()

                swap_out[j] = product.astype(BF16)

            @pl.when(j >= chips)
            def _():
                own_s[c % 2, j - chips] = product

            @pl.when((j >= 1) & (j <= chips))
            def _():
                swap(c, j - 1).start()

        lax.fori_loop(0, group, body, None)

    def chip_sum(c, j, r):
        return own_s[c % 2, j, r, :] + swap_in[c % 2, j, r, :].astype(F32)

    def scatter(c):
        residual(c).start()
        for j in range(chips):
            swap(c, j).wait_recv()

        @pl.when(c > 0)
        def _():
            for d in range(2):
                rs1(c - 1, d).wait_send()
                rs2(c - 1, d, 1 - d).wait_send()

        for d in range(2):

            def body(r, to):
                rs1_out[d, to, :] = chip_sum(c, OPP, r).astype(BF16)

            strips_of(d, body)
        for d in range(2):

            def body(r, to):
                rs2_out[d, r, :] = chip_sum(c, TOWARDS[d], r).astype(BF16)

            strips_of(1 - d, body)
        for d in range(2):
            rs1(c, d).start()
        for d in range(2):
            rs2(c, d, 1 - d).start()

    def add_on(c):
        for d in range(2):
            rs1(c, d).wait_recv()

            @pl.when(c > 0)
            def _():
                rs2(c - 1, d, d).wait_send()

            def body(r, to):
                rs2_out[d, r, :] = (chip_sum(c, TOWARDS[d], r) + rs1_in[c % 2, d, to, :].astype(F32)).astype(BF16)

            strips_of(d, body)
        for d in range(2):
            rs2(c, d, d).start()

    def finish(c):
        residual(c).wait()
        for d in range(2):
            for part in range(2):
                rs2(c, d, part).wait_recv()

        @pl.when(c > 0)
        def _():
            for d in range(2):
                for part in range(2):
                    ag1(c - 1, d, part).wait_send()
            pair(c - 1, SELF).wait_send()
            put(c - 1).wait()

        def body(r):
            total = chip_sum(c, SELF, r)
            for d in range(2):
                total += rs2_in[c % 2, d, r, :].astype(F32)
            fin_s[r, :] = (total + res_s[c % 2, r, :].astype(F32)).astype(BF16)

        strips(chunk, body)
        for other in range(2):
            for d in range(2):
                ag1(c, d, d if other == 0 else 1 - d).start()
        pair(c, SELF).start()
        put(c).start()

    def pass_on(c):
        for d in range(2):
            ag1(c, d, d).wait_recv()

            @pl.when(c > 0)
            def _():
                ag2(c - 1, d).wait_send()

            ag2(c, d).start()

    def give_partner(c):
        for d in range(2):
            ag1(c, d, 1 - d).wait_recv()

            @pl.when(c > 0)
            def _():
                pair(c - 1, FROM[d]).wait_send()

            pair(c, FROM[d]).start()
        for d in range(2):
            ag2(c, d).wait_recv()

        @pl.when(c > 0)
        def _():
            pair(c - 1, OPP).wait_send()
            for j in (LEFT, RIGHT, OPP):
                pair(c - 1, j).wait_recv()

        pair(c, OPP).start()

    barrier = pltpu.get_barrier_semaphore()
    load_x(0).start()
    for t in range(SLOTS - 1):
        fetch(0, t)
    for to in (*beside, partner):
        pl.semaphore_signal(barrier, inc=1, device_id=to, device_id_type=MESH)
    for h in range(heads):
        vt_s[h, HEAD:, :] = jnp.ones((ONES, rows), BF16)
    pl.semaphore_wait(barrier, 3)

    def step(c, _):
        new = c < chunks
        last = (c >= 1) & (c <= chunks)
        before = c >= 2

        @pl.when(new)
        def _():
            norm(c)
            project(c, 0)
            turn(c, q_s, 0)

        @pl.when(before)
        def _():
            finish(c - 2)

        @pl.when(new)
        def _():
            project(c, 1)
            turn(c, k_s, c * chunk)

        @pl.when(last)
        def _():
            add_on(c - 1)

        @pl.when(new)
        def _():
            project(c, 2)
            keep_values(c)
            attend(c)

        @pl.when(before)
        def _():
            pass_on(c - 2)
            pair(c - 2, SELF).wait_recv()

        @pl.when(new)
        def _():
            project_out(c)
            scatter(c)

        @pl.when(before)
        def _():
            give_partner(c - 2)

    lax.fori_loop(0, chunks + 2, step, None)

    c = chunks - 1
    for j in range(chips):
        swap(c, j).wait_send()
    for d in range(2):
        rs1(c, d).wait_send()
        ag2(c, d).wait_send()
        for part in range(2):
            rs2(c, d, part).wait_send()
            ag1(c, d, part).wait_send()
    put(c).wait()
    for j in range(chips):
        pair(c, j).wait_send()
    for j in (LEFT, RIGHT, OPP):
        pair(c, j).wait_recv()


def _tables(rows, chunk):
    half = HEAD // 2
    rate = float(THETA) ** (-np.arange(half) / half)

    def pairs(place):
        angle = place[:, None] * rate
        cos, sin = np.cos(angle), np.sin(angle)
        return np.concatenate([cos, cos], -1).astype(np.float32), np.concatenate([-sin, sin], -1).astype(np.float32)

    return *pairs(np.arange(chunk)), *pairs(np.arange(0, rows, chunk))


def solution(mesh):
    group = mesh.shape["tp"]

    def step(x, gain, wq, wk, wv, wo):
        rows, depth = x.shape
        wide = wq.shape[1]
        heads, piece = wide // HEAD, depth // group
        chunk = ROWS
        chunks, half = rows // chunk, chunk // 2
        kb = _fit(depth, 1024)
        blocks = depth // kb
        tables = _tables(rows, chunk)
        vmem, hbm = pl.BlockSpec(memory_space=pltpu.VMEM), pl.BlockSpec(memory_space=pl.ANY)
        dma = lambda *shape: pltpu.SemaphoreType.DMA(shape)
        return pl.pallas_call(
            functools.partial(_kernel, group),
            out_shape=jax.ShapeDtypeStruct((rows, depth), BF16),
            in_specs=[hbm, vmem, hbm, hbm, hbm, hbm, vmem, vmem, vmem, vmem],
            out_specs=hbm,
            scratch_shapes=[
                pltpu.VMEM((chunk, depth), BF16),
                pltpu.VMEM((blocks, chunk, kb), BF16),
                pltpu.VMEM((SLOTS, max(kb, wide), max(wide, piece)), BF16),
                pltpu.VMEM((chunk, wide), F32),
                pltpu.VMEM((heads, chunk, HEAD), BF16),
                pltpu.VMEM((heads, rows, HEAD), BF16),
                pltpu.VMEM((heads, HEAD + ONES, rows), BF16),
                pltpu.VMEM((heads, chunk), F32),
                pltpu.VMEM((heads, HEAD + ONES, chunk), F32),
                pltpu.VMEM((chunk, wide), BF16),
                pltpu.VMEM((2, group // 2, chunk, piece), F32),
                pltpu.VMEM((group // 2, chunk, piece), BF16),
                pltpu.VMEM((2, group // 2, chunk, piece), BF16),
                pltpu.VMEM((2, half, piece), BF16),
                pltpu.VMEM((2, 2, half, piece), BF16),
                pltpu.VMEM((2, chunk, piece), BF16),
                pltpu.VMEM((2, 2, chunk, piece), BF16),
                pltpu.VMEM((chunk, piece), BF16),
                pltpu.VMEM((2, chunk, piece), BF16),
                dma(SLOTS), pltpu.SemaphoreType.DMA, dma(2),
                dma(group // 2), dma(2, group // 2),
                dma(2), dma(2, 2),
                dma(2, 2), dma(2, 2, 2),
                dma(2, 2), dma(2, 2, 2),
                dma(2), dma(2, 2),
                dma(group // 2), dma(2, group // 2),
                pltpu.SemaphoreType.DMA,
            ],
            compiler_params=pltpu.CompilerParams(collective_id=0, has_side_effects=True, vmem_limit_bytes=62 * 2**20),
        )(x, gain.reshape(1, depth).astype(F32), wq, wk, wv, wo, *tables)

    tokens, columns = P("dp", None), P(None, "tp")
    return jax.shard_map(
        step,
        mesh=mesh,
        in_specs=(tokens, P(None), columns, columns, columns, P("tp", None)),
        out_specs=tokens,
        check_vma=False,
    )
```

```python
import functools

import jax
import jax.numpy as jnp
import numpy as np
from jax import lax
from jax.experimental import pallas as pl
from jax.experimental.pallas import tpu as pltpu
from jax.sharding import PartitionSpec as P

HEAD = 128
THETA = 10000
ROWS = 256
BLOCK = 1024
SLOTS = 3
STRIP = 32
ONES = 16
NEG = -1e30
HIDDEN = 2 * NEG
LOG2E = 1.4426950408889634
OPP, LEFT, SELF, RIGHT = range(4)
TOWARDS = (RIGHT, LEFT)
FROM = (LEFT, RIGHT)
MESH = pl.DeviceIdType.MESH
F32, BF16 = jnp.float32, jnp.bfloat16


def _fit(size, want, unit=128):
    return max(n for n in range(unit, want + 1, unit) if size % n == 0)


def _dot(a, b, ca, cb):
    return lax.dot_general(a, b, (((ca,), (cb,)), ((), ())), preferred_element_type=F32)


def _kernel(
    group, x_hbm, gain_ref, wq_hbm, wk_hbm, wv_hbm, wo_hbm, cb_ref, sb_ref, ca_ref, sa_ref, y_hbm,
    x_s, a_s, w_s, acc_s, q_s, k_s, vt_s, top_s, mix_s, seen_s, own_s, swap_out, swap_in, rs1_out, rs1_in, rs2_out, rs2_in, fin_s, res_s,
    w_sem, x_sem, res_sem, swap_ss, swap_rs, rs1_ss, rs1_rs, rs2_ss, rs2_rs, ag1_ss, ag1_rs, ag2_ss, ag2_rs, pair_ss, pair_rs, put_sem,
):
    rows, depth = x_hbm.shape
    wide = wq_hbm.shape[1]
    piece = depth // group
    heads = wide // HEAD
    chunk = x_s.shape[0]
    chunks = rows // chunk
    half = chunk // 2
    blocks, _, kb = a_s.shape
    tiles = blocks + group // 2
    e = HEAD**-0.5 * LOG2E

    me = lax.axis_index("tp")
    chips = group // 2
    chip, core = me // 2, me % 2
    places = [(chip + by) % chips for by in (2, chips - 1, 0, 1)]
    partner = {"tp": chip * 2 + 1 - core}
    beside = [{"tp": places[TOWARDS[d]] * 2 + core} for d in range(2)]

    def columns(place, whose):
        return pl.ds(pl.multiple_of((place * 2 + whose) * piece, piece), piece)

    def rows_of(c, part=None):
        if part is None:
            return pl.ds(pl.multiple_of(c * chunk, chunk), chunk)
        return pl.ds(pl.multiple_of(c * chunk + part * half, half), half)

    def part_rows(part):
        return pl.ds(part * half, half)

    def remote(src, dst, send, recv, to):
        return pltpu.make_async_remote_copy(src_ref=src, dst_ref=dst, send_sem=send, recv_sem=recv, device_id=to, device_id_type=MESH)

    def swap(c, j):
        return remote(swap_out.at[j], swap_in.at[c % 2, j], swap_ss.at[j], swap_rs.at[c % 2, j], partner)

    def rs1(c, d):
        return remote(rs1_out.at[d], rs1_in.at[c % 2, d], rs1_ss.at[d], rs1_rs.at[c % 2, d], beside[d])

    def rs2(c, d, part):
        return remote(
            rs2_out.at[d, part_rows(part)], rs2_in.at[c % 2, d, part_rows(part)], rs2_ss.at[d, part], rs2_rs.at[c % 2, d, part], beside[d]
        )

    def ag1(c, d, part):
        there = y_hbm.at[rows_of(c, part), columns(chip, core)]
        return remote(fin_s.at[part_rows(part)], there, ag1_ss.at[d, part], ag1_rs.at[c % 2, d, part], beside[d])

    def ag2(c, d):
        there = y_hbm.at[rows_of(c, d), columns(places[FROM[d]], core)]
        return remote(there, there, ag2_ss.at[d], ag2_rs.at[c % 2, d], beside[d])

    def pair(c, j):
        there = y_hbm.at[rows_of(c), columns(places[j], core)]
        return remote(fin_s if j == SELF else there, there, pair_ss.at[j], pair_rs.at[c % 2, j], partner)

    def put(c):
        return pltpu.make_async_copy(fin_s, y_hbm.at[rows_of(c), columns(chip, core)], put_sem)

    def residual(c):
        return pltpu.make_async_copy(x_hbm.at[rows_of(c), columns(chip, core)], res_s.at[c % 2], res_sem.at[c % 2])

    def load_x(c):
        return pltpu.make_async_copy(x_hbm.at[rows_of(c)], x_s, x_sem)

    def weight(i, n, slot):
        rows_here = pl.ds(pl.multiple_of(i * kb, kb), kb)
        there = w_s.at[slot, pl.ds(0, kb), pl.ds(n * wide, wide)]
        return pltpu.make_async_copy((wq_hbm, wk_hbm, wv_hbm)[n].at[rows_here], there, w_sem.at[slot, n])

    def out_weight(p, n, slot):
        j = p * 2 + n
        place = (chip + 2 + j) % chips
        whose = jnp.where(j < chips, 1 - core, core)
        there = w_s.at[slot, pl.ds(0, wide), pl.ds(n * piece, piece)]
        return pltpu.make_async_copy(wo_hbm.at[:, columns(place, whose)], there, w_sem.at[slot, n])

    def slot_of(c, t):
        return (c * tiles + t) % SLOTS

    def fetch(c, t):
        slot = slot_of(c, t)
        later = t >= tiles
        t = jnp.where(later, t - tiles, t)
        live = jnp.where(later, c + 1, c) < chunks

        @pl.when(live & (t < blocks))
        def _():
            for n in range(3):
                weight(t, n, slot).start()

        @pl.when(live & (t >= blocks))
        def _():
            for n in range(2):
                out_weight(t - blocks, n, slot).start()

    def strips(count, body):
        lax.fori_loop(0, count // STRIP, lambda r, _: body(pl.ds(pl.multiple_of(r * STRIP, STRIP), STRIP)), None)

    def strips_of(part, body):
        lax.fori_loop(
            0,
            half // STRIP,
            lambda r, _: body(pl.ds(pl.multiple_of(part * half + r * STRIP, STRIP), STRIP), pl.ds(pl.multiple_of(r * STRIP, STRIP), STRIP)),
            None,
        )

    def norm(c):
        load_x(c).wait()

        def body(r):
            total = jnp.zeros((STRIP, kb), F32)
            for i in range(blocks):
                part = x_s[r, i * kb : (i + 1) * kb].astype(F32)
                total += part * part
            scale = lax.rsqrt(jnp.sum(total, axis=-1, keepdims=True) / depth + 1e-6)
            for i in range(blocks):
                part = x_s[r, i * kb : (i + 1) * kb].astype(F32)
                a_s[i, r, :] = (part * scale * gain_ref[:, i * kb : (i + 1) * kb]).astype(BF16)

        strips(chunk, body)

        @pl.when(c + 1 < chunks)
        def _():
            load_x(c + 1).start()

    def project(c, first, last):
        def product(i):
            slot = slot_of(c, i)
            for n in range(3):
                weight(i, n, slot).wait()
            fetch(c, i + SLOTS - 1)
            return _dot(a_s[i], w_s[slot, :kb, : 3 * wide], 1, 0)

        def body(i, _):
            acc_s[...] += product(i)

        if first == 0:
            acc_s[...] = product(0)
        lax.fori_loop(max(first, 1), last, body, None)

    def turn(c, ref, at, n):
        ca, sa = ca_ref[pl.ds(c, 1), :], sa_ref[pl.ds(c, 1), :]

        def body(r):
            cb, sb = cb_ref[r, :], sb_ref[r, :]
            cos, sin = ca * cb - sa * sb, sa * cb + ca * sb
            for h in range(heads):
                t = acc_s[r, n * wide + h * HEAD : n * wide + (h + 1) * HEAD].astype(BF16).astype(F32)
                turned = t * cos + pltpu.roll(t, HEAD // 2, 1) * sin
                ref[h, pl.ds(pl.multiple_of(at + r.start, STRIP), STRIP), :] = turned.astype(BF16)

        strips(chunk, body)

    def keep_values(c):
        for h in range(heads):
            vt_s[h, :HEAD, rows_of(c)] = acc_s[:, 2 * wide + h * HEAD : 2 * wide + (h + 1) * HEAD].astype(BF16).T

    def attend(c):
        top_s[...] = jnp.full(top_s.shape, NEG, F32)
        mix_s[...] = jnp.zeros(mix_s.shape, F32)

        def block(j, masked):
            here = rows_of(j)
            scores = [_dot(k_s[h, here, :], q_s[h], 1, 1) for h in range(heads)]
            if masked:
                ok = lax.broadcasted_iota(jnp.int32, (chunk, chunk), 1) >= lax.broadcasted_iota(jnp.int32, (chunk, chunk), 0)
            weights, keeps = [], []
            for h, s in enumerate(scores):
                if masked:
                    s = jnp.where(ok, s, HIDDEN)
                old = top_s[h : h + 1, :]
                top = jnp.maximum(old, s.max(axis=0, keepdims=True))
                top_s[h : h + 1, :] = top
                weights.append(jnp.exp2((s - top) * e).astype(BF16))
                keeps.append(jnp.exp2((old - top) * e))
            for h in range(heads):
                mix_s[h] = mix_s[h] * keeps[h] + _dot(vt_s[h, :, here], weights[h], 1, 0)

        lax.fori_loop(0, c, lambda j, _: block(j, False), None)
        block(c, True)
        for h in range(heads):
            out = mix_s[h, :HEAD, :] * (1 / mix_s[h, HEAD : HEAD + 1, :])
            seen_s[:, h * HEAD : (h + 1) * HEAD] = out.T.astype(BF16)

    def project_out(c):
        def body(p, _):
            slot = slot_of(c, blocks + p)
            for n in range(2):
                out_weight(p, n, slot).wait()
            fetch(c, blocks + p + SLOTS - 1)
            product = _dot(seen_s[...], w_s[slot, :wide, : 2 * piece], 1, 0)

            @pl.when(p < chips // 2)
            def _():
                for n in range(2):

                    @pl.when(c > 0)
                    def _():
                        swap(c - 1, p * 2 + n).wait_send()

                    swap_out[p * 2 + n] = product[:, n * piece : (n + 1) * piece].astype(BF16)

            @pl.when(p >= chips // 2)
            def _():
                for n in range(2):
                    own_s[c % 2, p * 2 + n - chips] = product[:, n * piece : (n + 1) * piece]

            @pl.when((p >= 1) & (p <= chips // 2))
            def _():
                for n in range(2):
                    swap(c, p * 2 - 2 + n).start()

        lax.fori_loop(0, chips, body, None)

    def chip_sum(c, j, r):
        return own_s[c % 2, j, r, :] + swap_in[c % 2, j, r, :].astype(F32)

    def scatter(c):
        residual(c).start()
        for j in range(chips):
            swap(c, j).wait_recv()

        @pl.when(c > 0)
        def _():
            for d in range(2):
                rs1(c - 1, d).wait_send()
                rs2(c - 1, d, 1 - d).wait_send()

        for d in range(2):

            def body(r, to):
                rs1_out[d, to, :] = chip_sum(c, OPP, r).astype(BF16)

            strips_of(d, body)
        for d in range(2):

            def body(r, to):
                rs2_out[d, r, :] = chip_sum(c, TOWARDS[d], r).astype(BF16)

            strips_of(1 - d, body)
        for d in range(2):
            rs1(c, d).start()
        for d in range(2):
            rs2(c, d, 1 - d).start()

    def add_on(c):
        for d in range(2):
            rs1(c, d).wait_recv()

            @pl.when(c > 0)
            def _():
                rs2(c - 1, d, d).wait_send()

            def body(r, to):
                rs2_out[d, r, :] = (chip_sum(c, TOWARDS[d], r) + rs1_in[c % 2, d, to, :].astype(F32)).astype(BF16)

            strips_of(d, body)
        for d in range(2):
            rs2(c, d, d).start()

    def finish(c):
        residual(c).wait()
        for d in range(2):
            for part in range(2):
                rs2(c, d, part).wait_recv()

        @pl.when(c > 0)
        def _():
            for d in range(2):
                for part in range(2):
                    ag1(c - 1, d, part).wait_send()
            pair(c - 1, SELF).wait_send()
            put(c - 1).wait()

        def body(r):
            total = chip_sum(c, SELF, r)
            for d in range(2):
                total += rs2_in[c % 2, d, r, :].astype(F32)
            fin_s[r, :] = (total + res_s[c % 2, r, :].astype(F32)).astype(BF16)

        strips(chunk, body)
        for other in range(2):
            for d in range(2):
                ag1(c, d, d if other == 0 else 1 - d).start()
        pair(c, SELF).start()
        put(c).start()

    def pass_on(c):
        for d in range(2):
            ag1(c, d, d).wait_recv()

            @pl.when(c > 0)
            def _():
                ag2(c - 1, d).wait_send()

            ag2(c, d).start()

    def give_partner(c):
        for d in range(2):
            ag1(c, d, 1 - d).wait_recv()

            @pl.when(c > 0)
            def _():
                pair(c - 1, FROM[d]).wait_send()

            pair(c, FROM[d]).start()
        for d in range(2):
            ag2(c, d).wait_recv()

        @pl.when(c > 0)
        def _():
            pair(c - 1, OPP).wait_send()

        pair(c, OPP).start()

    barrier = pltpu.get_barrier_semaphore()
    load_x(0).start()
    for t in range(SLOTS - 1):
        fetch(0, t)
    for to in (*beside, partner):
        pl.semaphore_signal(barrier, inc=1, device_id=to, device_id_type=MESH)
    for h in range(heads):
        vt_s[h, HEAD:, :] = jnp.ones((ONES, rows), BF16)
    pl.semaphore_wait(barrier, 3)

    def step(c, _):
        new = c < chunks
        last = (c >= 1) & (c <= chunks)
        before = c >= 2
        early = blocks // 2

        @pl.when(new)
        def _():
            norm(c)
            project(c, 0, early)

        @pl.when(last)
        def _():
            add_on(c - 1)

        @pl.when(before)
        def _():
            pass_on(c - 2)

        @pl.when(c >= 3)
        def _():
            for j in (LEFT, RIGHT, OPP):
                pair(c - 3, j).wait_recv()

        @pl.when(new)
        def _():
            project(c, early, blocks)
            turn(c, q_s, 0, 0)
            turn(c, k_s, c * chunk, 1)
            keep_values(c)

        @pl.when(last)
        def _():
            finish(c - 1)

        @pl.when(new)
        def _():
            attend(c)

        @pl.when(before)
        def _():
            pair(c - 2, SELF).wait_recv()

        @pl.when(new)
        def _():
            project_out(c)
            scatter(c)

        @pl.when(before)
        def _():
            give_partner(c - 2)

    lax.fori_loop(0, chunks + 2, step, None)

    c = chunks - 1
    for j in range(chips):
        swap(c, j).wait_send()
    for d in range(2):
        rs1(c, d).wait_send()
        ag2(c, d).wait_send()
        for part in range(2):
            rs2(c, d, part).wait_send()
            ag1(c, d, part).wait_send()
    put(c).wait()
    for j in range(chips):
        pair(c, j).wait_send()
    for j in (LEFT, RIGHT, OPP):
        pair(c, j).wait_recv()


def _tables(rows, chunk):
    half = HEAD // 2
    rate = float(THETA) ** (-np.arange(half) / half)

    def pairs(place):
        angle = place[:, None] * rate
        cos, sin = np.cos(angle), np.sin(angle)
        return np.concatenate([cos, cos], -1).astype(np.float32), np.concatenate([-sin, sin], -1).astype(np.float32)

    return *pairs(np.arange(chunk)), *pairs(np.arange(0, rows, chunk))


def solution(mesh):
    group = mesh.shape["tp"]

    def step(x, gain, wq, wk, wv, wo):
        rows, depth = x.shape
        wide = wq.shape[1]
        heads, piece = wide // HEAD, depth // group
        chunk = ROWS
        chunks, half = rows // chunk, chunk // 2
        kb = _fit(depth, BLOCK)
        blocks = depth // kb
        tables = _tables(rows, chunk)
        vmem, hbm = pl.BlockSpec(memory_space=pltpu.VMEM), pl.BlockSpec(memory_space=pl.ANY)
        dma = lambda *shape: pltpu.SemaphoreType.DMA(shape)
        return pl.pallas_call(
            functools.partial(_kernel, group),
            out_shape=jax.ShapeDtypeStruct((rows, depth), BF16),
            in_specs=[hbm, vmem, hbm, hbm, hbm, hbm, vmem, vmem, vmem, vmem],
            out_specs=hbm,
            scratch_shapes=[
                pltpu.VMEM((chunk, depth), BF16),
                pltpu.VMEM((blocks, chunk, kb), BF16),
                pltpu.VMEM((SLOTS, max(kb, wide), max(3 * wide, 2 * piece)), BF16),
                pltpu.VMEM((chunk, 3 * wide), F32),
                pltpu.VMEM((heads, chunk, HEAD), BF16),
                pltpu.VMEM((heads, rows, HEAD), BF16),
                pltpu.VMEM((heads, HEAD + ONES, rows), BF16),
                pltpu.VMEM((heads, chunk), F32),
                pltpu.VMEM((heads, HEAD + ONES, chunk), F32),
                pltpu.VMEM((chunk, wide), BF16),
                pltpu.VMEM((2, group // 2, chunk, piece), F32),
                pltpu.VMEM((group // 2, chunk, piece), BF16),
                pltpu.VMEM((2, group // 2, chunk, piece), BF16),
                pltpu.VMEM((2, half, piece), BF16),
                pltpu.VMEM((2, 2, half, piece), BF16),
                pltpu.VMEM((2, chunk, piece), BF16),
                pltpu.VMEM((2, 2, chunk, piece), BF16),
                pltpu.VMEM((chunk, piece), BF16),
                pltpu.VMEM((2, chunk, piece), BF16),
                dma(SLOTS, 3), pltpu.SemaphoreType.DMA, dma(2),
                dma(group // 2), dma(2, group // 2),
                dma(2), dma(2, 2),
                dma(2, 2), dma(2, 2, 2),
                dma(2, 2), dma(2, 2, 2),
                dma(2), dma(2, 2),
                dma(group // 2), dma(2, group // 2),
                pltpu.SemaphoreType.DMA,
            ],
            compiler_params=pltpu.CompilerParams(collective_id=0, has_side_effects=True, vmem_limit_bytes=62 * 2**20),
        )(x, gain.reshape(1, depth).astype(F32), wq, wk, wv, wo, *tables)

    tokens, columns = P("dp", None), P(None, "tp")
    return jax.shard_map(
        step,
        mesh=mesh,
        in_specs=(tokens, P(None), columns, columns, columns, P("tp", None)),
        out_specs=tokens,
        check_vma=False,
    )
```

```python
import functools

import jax
import jax.numpy as jnp
import numpy as np
from jax import lax
from jax.experimental import pallas as pl
from jax.experimental.pallas import tpu as pltpu
from jax.sharding import PartitionSpec as P

HEAD = 128
THETA = 10000
ROWS = 256
BLOCK = 1024
SLOTS = 3
X_PARTS = 4
STRIP = 32
SPLIT = 20
ONES = 16
NEG = -1e30
HIDDEN = 2 * NEG
LOG2E = 1.4426950408889634
OPP, LEFT, SELF, RIGHT = range(4)
TOWARDS = (RIGHT, LEFT)
FROM = (LEFT, RIGHT)
MESH = pl.DeviceIdType.MESH
F32, BF16 = jnp.float32, jnp.bfloat16


def _fit(size, want, unit=128):
    return max(n for n in range(unit, want + 1, unit) if size % n == 0)


def _dot(a, b, ca, cb):
    return lax.dot_general(a, b, (((ca,), (cb,)), ((), ())), preferred_element_type=F32)


def _kernel(
    group, x_hbm, gain_ref, wq_hbm, wk_hbm, wv_hbm, wo_hbm, cb_ref, sb_ref, ca_ref, sa_ref, y_hbm, fin_hbm,
    x_s, a_s, w_s, acc_s, q_s, k_s, vt_s, top_s, mix_s, seen_s, own_s, swap_out, swap_in, rs1_out, rs1_in, rs2_out, rs2_in, fin_s, res_s,
    w_sem, x_sem, res_sem, swap_ss, swap_rs, rs1_ss, rs1_rs, rs2_ss, rs2_rs, ag1_ss, ag1_rs, ag2_ss, ag2_rs, pair_ss, pair_rs, put_sem,
):
    rows, depth = x_hbm.shape
    wide = wq_hbm.shape[1]
    piece = depth // group
    heads = wide // HEAD
    chunk = x_s.shape[0]
    chunks = rows // chunk
    half = chunk // 2
    blocks, _, kb = a_s.shape
    tiles = blocks + group // 2
    e = HEAD**-0.5 * LOG2E

    me = lax.axis_index("tp")
    chips = group // 2
    chip, core = me // 2, me % 2
    places = [(chip + by) % chips for by in (2, chips - 1, 0, 1)]
    partner = {"tp": chip * 2 + 1 - core}
    beside = [{"tp": places[TOWARDS[d]] * 2 + core} for d in range(2)]

    def columns(place, whose):
        return pl.ds(pl.multiple_of((place * 2 + whose) * piece, piece), piece)

    def rows_of(c, part=None):
        if part is None:
            return pl.ds(pl.multiple_of(c * chunk, chunk), chunk)
        return pl.ds(pl.multiple_of(c * chunk + part * half, half), half)

    def part_rows(part):
        return pl.ds(part * half, half)

    def remote(src, dst, send, recv, to):
        return pltpu.make_async_remote_copy(src_ref=src, dst_ref=dst, send_sem=send, recv_sem=recv, device_id=to, device_id_type=MESH)

    def swap(c, j):
        return remote(swap_out.at[j], swap_in.at[c % 2, j], swap_ss.at[j], swap_rs.at[c % 2, j], partner)

    def rs1(c, d):
        return remote(rs1_out.at[d], rs1_in.at[c % 2, d], rs1_ss.at[d], rs1_rs.at[c % 2, d], beside[d])

    def rs2(c, d, part):
        return remote(
            rs2_out.at[d, part_rows(part)], rs2_in.at[c % 2, d, part_rows(part)], rs2_ss.at[d, part], rs2_rs.at[c % 2, d, part], beside[d]
        )

    def ag1(c, d, part):
        there = y_hbm.at[rows_of(c, part), columns(chip, core)]
        return remote(fin_s.at[part_rows(part)], there, ag1_ss.at[d, part], ag1_rs.at[c % 2, d, part], beside[d])

    def ag2(c, d):
        there = y_hbm.at[rows_of(c, d), columns(places[FROM[d]], core)]
        return remote(there, there, ag2_ss.at[d], ag2_rs.at[c % 2, d], beside[d])

    def pair(c, j):
        there = y_hbm.at[rows_of(c), columns(places[j], core)]
        return remote(fin_s if j == SELF else there, there, pair_ss.at[j], pair_rs.at[c % 2, j], partner)

    def put(c):
        return pltpu.make_async_copy(fin_s, y_hbm.at[rows_of(c), columns(chip, core)], put_sem)

    def put_last():
        return pltpu.make_async_copy(fin_s, fin_hbm, put_sem)

    def residual(c):
        return pltpu.make_async_copy(x_hbm.at[rows_of(c), columns(chip, core)], res_s.at[c % 2], res_sem.at[c % 2])

    def load_x(c, part):
        rows_here = pl.ds(pl.multiple_of(c * chunk + part * (chunk // X_PARTS), chunk // X_PARTS), chunk // X_PARTS)
        return pltpu.make_async_copy(x_hbm.at[rows_here], x_s.at[pl.ds(part * (chunk // X_PARTS), chunk // X_PARTS)], x_sem.at[part])

    def weight(i, n, slot):
        rows_here = pl.ds(pl.multiple_of(i * kb, kb), kb)
        there = w_s.at[slot, pl.ds(0, kb), pl.ds(n * wide, wide)]
        return pltpu.make_async_copy((wq_hbm, wk_hbm, wv_hbm)[n].at[rows_here], there, w_sem.at[slot, n])

    def out_weight(p, n, slot):
        j = p * 2 + n
        place = (chip + 2 + j) % chips
        whose = jnp.where(j < chips, 1 - core, core)
        there = w_s.at[slot, pl.ds(0, wide), pl.ds(n * piece, piece)]
        return pltpu.make_async_copy(wo_hbm.at[:, columns(place, whose)], there, w_sem.at[slot, n])

    def slot_of(c, t):
        return (c * tiles + t) % SLOTS

    def fetch(c, t):
        slot = slot_of(c, t)
        later = t >= tiles
        t = jnp.where(later, t - tiles, t)
        live = jnp.where(later, c + 1, c) < chunks

        @pl.when(live & (t < blocks))
        def _():
            for n in range(3):
                weight(t, n, slot).start()

        @pl.when(live & (t >= blocks))
        def _():
            for n in range(2):
                out_weight(t - blocks, n, slot).start()

    def strips(count, body):
        lax.fori_loop(0, count // STRIP, lambda r, _: body(pl.ds(pl.multiple_of(r * STRIP, STRIP), STRIP)), None)

    def strips_of(part, body):
        lax.fori_loop(
            0,
            half // STRIP,
            lambda r, _: body(pl.ds(pl.multiple_of(part * half + r * STRIP, STRIP), STRIP), pl.ds(pl.multiple_of(r * STRIP, STRIP), STRIP)),
            None,
        )

    def norm(c):
        def body(r):
            total = jnp.zeros((STRIP, kb), F32)
            for i in range(blocks):
                part = x_s[r, i * kb : (i + 1) * kb].astype(F32)
                total += part * part
            scale = lax.rsqrt(jnp.sum(total, axis=-1, keepdims=True) / depth + 1e-6)
            for i in range(blocks):
                part = x_s[r, i * kb : (i + 1) * kb].astype(F32)
                a_s[i, r, :] = (part * scale * gain_ref[:, i * kb : (i + 1) * kb]).astype(BF16)

        each = chunk // X_PARTS // STRIP
        for part in range(X_PARTS):
            load_x(c, part).wait()
            lax.fori_loop(part * each, (part + 1) * each, lambda r, _: body(pl.ds(pl.multiple_of(r * STRIP, STRIP), STRIP)), None)

        @pl.when(c + 1 < chunks)
        def _():
            for part in range(X_PARTS):
                load_x(c + 1, part).start()

    def project(c, first, last):
        def product(i):
            slot = slot_of(c, i)
            for n in range(3):
                weight(i, n, slot).wait()
            fetch(c, i + SLOTS - 1)
            return _dot(a_s[i], w_s[slot, :kb, : 3 * wide], 1, 0)

        def body(i, _):
            acc_s[...] += product(i)

        if first == 0:
            acc_s[...] = product(0)
        lax.fori_loop(max(first, 1), last, body, None)

    def turn(c, ref, at, n):
        ca, sa = ca_ref[pl.ds(c, 1), :], sa_ref[pl.ds(c, 1), :]

        def body(r):
            cb, sb = cb_ref[r, :], sb_ref[r, :]
            cos, sin = ca * cb - sa * sb, sa * cb + ca * sb
            for h in range(heads):
                t = acc_s[r, n * wide + h * HEAD : n * wide + (h + 1) * HEAD].astype(BF16).astype(F32)
                turned = t * cos + pltpu.roll(t, HEAD // 2, 1) * sin
                ref[h, pl.ds(pl.multiple_of(at + r.start, STRIP), STRIP), :] = turned.astype(BF16)

        strips(chunk, body)

    def keep_values(c):
        for h in range(heads):
            vt_s[h, :HEAD, rows_of(c)] = acc_s[:, 2 * wide + h * HEAD : 2 * wide + (h + 1) * HEAD].astype(BF16).T

    def attend(c):
        top_s[...] = jnp.full(top_s.shape, NEG, F32)
        mix_s[...] = jnp.zeros(mix_s.shape, F32)

        def block(j, masked):
            here = rows_of(j)
            scores = [_dot(k_s[h, here, :], q_s[h], 1, 1) for h in range(heads)]
            if masked:
                ok = lax.broadcasted_iota(jnp.int32, (chunk, chunk), 1) >= lax.broadcasted_iota(jnp.int32, (chunk, chunk), 0)
            weights, keeps = [], []
            for h, s in enumerate(scores):
                if masked:
                    s = jnp.where(ok, s, HIDDEN)
                old = top_s[h : h + 1, :]
                top = jnp.maximum(old, s.max(axis=0, keepdims=True))
                top_s[h : h + 1, :] = top
                weights.append(jnp.exp2((s - top) * e).astype(BF16))
                keeps.append(jnp.exp2((old - top) * e))
            for h in range(heads):
                mix_s[h] = mix_s[h] * keeps[h] + _dot(vt_s[h, :, here], weights[h], 1, 0)

        lax.fori_loop(0, c, lambda j, _: block(j, False), None)
        block(c, True)
        for h in range(heads):
            out = mix_s[h, :HEAD, :] * (1 / mix_s[h, HEAD : HEAD + 1, :])
            seen_s[:, h * HEAD : (h + 1) * HEAD] = out.T.astype(BF16)

    def project_out(c):
        for p in range(chips):
            if p == chips - 1:
                scatter_opposite(c)
            slot = slot_of(c, blocks + p)
            for n in range(2):
                out_weight(p, n, slot).wait()
            fetch(c, blocks + p + SLOTS - 1)
            product = _dot(seen_s[...], w_s[slot, :wide, : 2 * piece], 1, 0)
            for n in range(2):
                j = p * 2 + n
                part = product[:, n * piece : (n + 1) * piece]
                if j < chips:

                    @pl.when(c > 0)
                    def _():
                        swap(c - 1, j).wait_send()

                    swap_out[j] = part.astype(BF16)
                else:
                    own_s[c % 2, j - chips] = part
            if 1 <= p <= chips // 2:
                for n in range(2):
                    swap(c, p * 2 - 2 + n).start()

    def chip_sum(c, j, r):
        return own_s[c % 2, j, r, :] + swap_in[c % 2, j, r, :].astype(F32)

    def scatter_opposite(c):
        residual(c).start()
        swap(c, OPP).wait_recv()

        @pl.when(c > 0)
        def _():
            for d in range(2):
                rs1(c - 1, d).wait_send()

        for d in range(2):

            def body(r, to):
                rs1_out[d, to, :] = chip_sum(c, OPP, r).astype(BF16)

            strips_of(d, body)
        for d in range(2):
            rs1(c, d).start()

    def scatter(c):
        for j in (LEFT, SELF, RIGHT):
            swap(c, j).wait_recv()

        @pl.when(c > 0)
        def _():
            for d in range(2):
                rs2(c - 1, d, 1 - d).wait_send()

        for d in range(2):

            def body(r, to):
                rs2_out[d, r, :] = chip_sum(c, TOWARDS[d], r).astype(BF16)

            strips_of(1 - d, body)
        for d in range(2):
            rs2(c, d, 1 - d).start()

    def add_on(c):
        for d in range(2):
            rs1(c, d).wait_recv()

            @pl.when(c > 0)
            def _():
                rs2(c - 1, d, d).wait_send()

            def body(r, to):
                rs2_out[d, r, :] = (chip_sum(c, TOWARDS[d], r) + rs1_in[c % 2, d, to, :].astype(F32)).astype(BF16)

            strips_of(d, body)
        for d in range(2):
            rs2(c, d, d).start()

    def finish(c):
        residual(c).wait()
        for d in range(2):
            for part in range(2):
                rs2(c, d, part).wait_recv()

        @pl.when(c > 0)
        def _():
            for d in range(2):
                for part in range(2):
                    ag1(c - 1, d, part).wait_send()
            pair(c - 1, SELF).wait_send()
            put(c - 1).wait()

        def body(r):
            total = chip_sum(c, SELF, r)
            for d in range(2):
                total += rs2_in[c % 2, d, r, :].astype(F32)
            fin_s[r, :] = (total + res_s[c % 2, r, :].astype(F32)).astype(BF16)

        strips(chunk, body)

        @pl.when(c < chunks - 1)
        def _():
            for other in range(2):
                for d in range(2):
                    ag1(c, d, d if other == 0 else 1 - d).start()
            pair(c, SELF).start()
            put(c).start()

        @pl.when(c == chunks - 1)
        def _():
            put_last().start()

    def pass_on(c):
        for d in range(2):
            ag1(c, d, d).wait_recv()

            @pl.when(c > 0)
            def _():
                ag2(c - 1, d).wait_send()

            ag2(c, d).start()

    def give_partner(c):
        for d in range(2):
            ag1(c, d, 1 - d).wait_recv()

            @pl.when(c > 0)
            def _():
                pair(c - 1, FROM[d]).wait_send()

            pair(c, FROM[d]).start()
        for d in range(2):
            ag2(c, d).wait_recv()

        @pl.when(c > 0)
        def _():
            pair(c - 1, OPP).wait_send()

        pair(c, OPP).start()

    barrier = pltpu.get_barrier_semaphore()
    for part in range(X_PARTS):
        load_x(0, part).start()
    for t in range(SLOTS - 1):
        fetch(0, t)
    for to in (*beside, partner):
        pl.semaphore_signal(barrier, inc=1, device_id=to, device_id_type=MESH)
    for h in range(heads):
        vt_s[h, HEAD:, :] = jnp.ones((ONES, rows), BF16)
    pl.semaphore_wait(barrier, 3)

    def step(c, _):
        new = c < chunks
        last = (c >= 1) & (c <= chunks)
        before = c >= 2
        early = blocks // 2

        @pl.when(new)
        def _():
            norm(c)
            project(c, 0, early)

        @pl.when(last)
        def _():
            add_on(c - 1)

        @pl.when(before)
        def _():
            pass_on(c - 2)

        @pl.when(c >= 3)
        def _():
            for j in (LEFT, RIGHT, OPP):
                pair(c - 3, j).wait_recv()

        @pl.when(new)
        def _():
            project(c, early, blocks)
            turn(c, q_s, 0, 0)
            turn(c, k_s, c * chunk, 1)
            keep_values(c)

        @pl.when(last)
        def _():
            finish(c - 1)

        @pl.when(new)
        def _():
            attend(c)

        @pl.when(before)
        def _():
            pair(c - 2, SELF).wait_recv()

        @pl.when(new)
        def _():
            project_out(c)
            scatter(c)

        @pl.when(before)
        def _():
            give_partner(c - 2)

    lax.fori_loop(0, chunks + 1, step, None)

    c = chunks - 1
    for j in range(chips):
        swap(c, j).wait_send()
    for d in range(2):
        rs1(c, d).wait_send()
        ag2(c - 1, d).wait_send()
        for part in range(2):
            rs2(c, d, part).wait_send()
    put_last().wait()
    for j in (LEFT, RIGHT, OPP):
        pair(c - 1, j).wait_send()
        pair(c - 1, j).wait_recv()


def _copy_kernel(first, count, *refs):
    src, dst, buf, in_sem, out_sem = refs[0], refs[-4], *refs[-3:]
    slots, each = buf.shape[:2]

    def take(i):
        return pltpu.make_async_copy(src.at[pl.ds((first + i) * each, each)], buf.at[i % slots], in_sem.at[i % slots])

    def give(i):
        return pltpu.make_async_copy(buf.at[i % slots], dst.at[pl.ds((first + i) * each, each)], out_sem.at[i % slots])

    ahead = slots // 2
    for i in range(min(ahead, count)):
        take(i).start()
    for i in range(count):
        take(i).wait()
        give(i).start()
        if i + ahead < count:
            if i + ahead >= slots:
                give(i + ahead - slots).wait()
            take(i + ahead).start()
    for i in range(max(count - slots, 0), count):
        give(i).wait()


def _copy_rows(src, first, count, each, into=None):
    hbm = pl.BlockSpec(memory_space=pl.ANY)
    given = (src,) if into is None else (src, into)
    slots = 16
    return pl.pallas_call(
        functools.partial(_copy_kernel, first, count),
        out_shape=jax.ShapeDtypeStruct(src.shape, src.dtype),
        in_specs=[hbm] * len(given),
        out_specs=hbm,
        scratch_shapes=[
            pltpu.VMEM((slots, each, src.shape[1]), src.dtype), pltpu.SemaphoreType.DMA((slots,)), pltpu.SemaphoreType.DMA((slots,)),
        ],
        input_output_aliases={} if into is None else {1: 0},
        compiler_params=pltpu.CompilerParams(vmem_limit_bytes=40 * 2**20),
        cost_estimate=pl.CostEstimate(flops=count * each * src.shape[1] * 200, bytes_accessed=count * each * src.shape[1] * 4, transcendentals=0),
    )(*given)


def _place_kernel(group, _, *refs):
    pieces, out, sem = refs[:-2], refs[-2], refs[-1]
    me = lax.axis_index("tp")
    chips = group // 2
    chip, core = me // 2, me % 2
    places = [(chip + by) % chips for by in (2, 2, chips - 1, 0, 1)]
    rows = out.shape[0]
    chunk, piece = pieces[2].shape
    copies = []
    for n, ref in enumerate(pieces):
        j = n % 5
        at = rows - chunk + (chunk // 2 if j == 1 else 0)
        whose = core if n < 5 else 1 - core
        columns = pl.ds(pl.multiple_of((places[j] * 2 + whose) * piece, piece), piece)
        copies.append(pltpu.make_async_copy(ref, out.at[pl.ds(at, ref.shape[0]), columns], sem.at[n]))
    for copy in copies:
        copy.start()
    for copy in copies:
        copy.wait()


def _place(group, y, pieces):
    hbm, vmem = pl.BlockSpec(memory_space=pl.ANY), pl.BlockSpec(memory_space=pltpu.VMEM)
    return pl.pallas_call(
        functools.partial(_place_kernel, group),
        out_shape=jax.ShapeDtypeStruct(y.shape, y.dtype),
        in_specs=[hbm] + [vmem] * len(pieces),
        out_specs=hbm,
        scratch_shapes=[pltpu.SemaphoreType.DMA((len(pieces),))],
        input_output_aliases={0: 0},
        compiler_params=pltpu.CompilerParams(vmem_limit_bytes=16 * 2**20),
        cost_estimate=pl.CostEstimate(flops=10**6, bytes_accessed=10**7, transcendentals=0),
    )(y, *pieces)


def _tables(rows, chunk):
    half = HEAD // 2
    rate = float(THETA) ** (-np.arange(half) / half)

    def pairs(place):
        angle = place[:, None] * rate
        cos, sin = np.cos(angle), np.sin(angle)
        return np.concatenate([cos, cos], -1).astype(np.float32), np.concatenate([-sin, sin], -1).astype(np.float32)

    return *pairs(np.arange(chunk)), *pairs(np.arange(0, rows, chunk))


def solution(mesh):
    group = mesh.shape["tp"]

    def step(x, gain, wq, wk, wv, wo):
        rows, depth = x.shape
        wide = wq.shape[1]
        heads, piece = wide // HEAD, depth // group
        chunk = ROWS
        chunks, half = rows // chunk, chunk // 2
        kb = _fit(depth, BLOCK)
        blocks = depth // kb
        tables = _tables(rows, chunk)
        vmem, hbm = pl.BlockSpec(memory_space=pltpu.VMEM), pl.BlockSpec(memory_space=pl.ANY)
        dma = lambda *shape: pltpu.SemaphoreType.DMA(shape)
        early, done = pl.pallas_call(
            functools.partial(_kernel, group),
            out_shape=[jax.ShapeDtypeStruct((rows, depth), BF16), jax.ShapeDtypeStruct((chunk, piece), BF16)],
            in_specs=[hbm, vmem, hbm, hbm, hbm, hbm, vmem, vmem, vmem, vmem],
            out_specs=[hbm, hbm],
            scratch_shapes=[
                pltpu.VMEM((chunk, depth), BF16),
                pltpu.VMEM((blocks, chunk, kb), BF16),
                pltpu.VMEM((SLOTS, max(kb, wide), max(3 * wide, 2 * piece)), BF16),
                pltpu.VMEM((chunk, 3 * wide), F32),
                pltpu.VMEM((heads, chunk, HEAD), BF16),
                pltpu.VMEM((heads, rows, HEAD), BF16),
                pltpu.VMEM((heads, HEAD + ONES, rows), BF16),
                pltpu.VMEM((heads, chunk), F32),
                pltpu.VMEM((heads, HEAD + ONES, chunk), F32),
                pltpu.VMEM((chunk, wide), BF16),
                pltpu.VMEM((2, group // 2, chunk, piece), F32),
                pltpu.VMEM((group // 2, chunk, piece), BF16),
                pltpu.VMEM((2, group // 2, chunk, piece), BF16),
                pltpu.VMEM((2, half, piece), BF16),
                pltpu.VMEM((2, 2, half, piece), BF16),
                pltpu.VMEM((2, chunk, piece), BF16),
                pltpu.VMEM((2, 2, chunk, piece), BF16),
                pltpu.VMEM((chunk, piece), BF16),
                pltpu.VMEM((2, chunk, piece), BF16),
                dma(SLOTS, 3), dma(X_PARTS), dma(2),
                dma(group // 2), dma(2, group // 2),
                dma(2), dma(2, 2),
                dma(2, 2), dma(2, 2, 2),
                dma(2, 2), dma(2, 2, 2),
                dma(2), dma(2, 2),
                dma(group // 2), dma(2, group // 2),
                pltpu.SemaphoreType.DMA,
            ],
            compiler_params=pltpu.CompilerParams(collective_id=0, has_side_effects=True, vmem_limit_bytes=62 * 2**20),
        )(x, gain.reshape(1, depth).astype(F32), wq, wk, wv, wo, *tables)

        right = [(i, (i + 2) % group) for i in range(group)]
        left = [(i, (i - 2) % group) for i in range(group)]
        other = [(i, i + 1 - 2 * (i % 2)) for i in range(group)]
        send = lambda t, to: lax.ppermute(t, "tp", to)
        from_left, from_right, theirs = send(done, right), send(done, left), send(done, other)
        each = chunk // 4
        count = (chunks - 1) * 4
        y = _copy_rows(early, 0, SPLIT, each)
        y, from_left, from_right = lax.optimization_barrier((y, from_left, from_right))
        opp_a, opp_b = send(from_left[:half], right), send(from_right[half:], left)
        sides = send(from_left, other), send(from_right, other)
        y = _copy_rows(early, SPLIT, count - SPLIT, each, y)
        y, opp_a, opp_b = lax.optimization_barrier((y, opp_a, opp_b))
        mine = (opp_a, opp_b, from_left, done, from_right)
        given = (send(opp_a, other), send(opp_b, other), sides[0], theirs, sides[1])
        return _place(group, y, [*mine, *given])

    tokens, columns = P("dp", None), P(None, "tp")
    return jax.shard_map(
        step,
        mesh=mesh,
        in_specs=(tokens, P(None), columns, columns, columns, P("tp", None)),
        out_specs=tokens,
        check_vma=False,
    )
```

```python
import functools

import jax
import jax.numpy as jnp
import numpy as np
from jax import lax
from jax.experimental import pallas as pl
from jax.experimental.pallas import tpu as pltpu
from jax.sharding import PartitionSpec as P

HEAD = 128
THETA = 10000
ROWS = 256
BLOCK = 1024
SLOTS = 3
X_PARTS = 4
STRIP = 32
SPLIT = 22
ONES = 16
NEG = -1e30
HIDDEN = 2 * NEG
LOG2E = 1.4426950408889634
OPP, LEFT, SELF, RIGHT = range(4)
TOWARDS = (RIGHT, LEFT)
FROM = (LEFT, RIGHT)
MESH = pl.DeviceIdType.MESH
F32, BF16 = jnp.float32, jnp.bfloat16


def _fit(size, want, unit=128):
    return max(n for n in range(unit, want + 1, unit) if size % n == 0)


def _dot(a, b, ca, cb):
    return lax.dot_general(a, b, (((ca,), (cb,)), ((), ())), preferred_element_type=F32)


def _kernel(
    group, x_hbm, gain_ref, wq_hbm, wk_hbm, wv_hbm, wo_hbm, cb_ref, sb_ref, ca_ref, sa_ref, y_hbm, fin_hbm,
    x_s, a_s, w_s, acc_s, q_s, k_s, vt_s, top_s, mix_s, seen_s, own_s, swap_out, swap_in, rs1_out, rs1_in, rs2_out, rs2_in, fin_s, res_s, gain_s,
    w_sem, x_sem, res_sem, swap_ss, swap_rs, rs1_ss, rs1_rs, rs2_ss, rs2_rs, ag1_ss, ag1_rs, ag2_ss, ag2_rs, pair_ss, pair_rs, put_sem,
):
    rows, depth = x_hbm.shape
    wide = wq_hbm.shape[1]
    piece = depth // group
    heads = wide // HEAD
    chunk = x_s.shape[0]
    chunks = rows // chunk
    half = chunk // 2
    blocks, _, kb = a_s.shape
    tiles = blocks + group // 2
    e = HEAD**-0.5 * LOG2E

    me = lax.axis_index("tp")
    chips = group // 2
    chip, core = me // 2, me % 2
    places = [(chip + by) % chips for by in (2, chips - 1, 0, 1)]
    partner = {"tp": chip * 2 + 1 - core}
    beside = [{"tp": places[TOWARDS[d]] * 2 + core} for d in range(2)]

    def columns(place, whose):
        return pl.ds(pl.multiple_of((place * 2 + whose) * piece, piece), piece)

    def rows_of(c, part=None):
        if part is None:
            return pl.ds(pl.multiple_of(c * chunk, chunk), chunk)
        return pl.ds(pl.multiple_of(c * chunk + part * half, half), half)

    def part_rows(part):
        return pl.ds(part * half, half)

    def remote(src, dst, send, recv, to):
        return pltpu.make_async_remote_copy(src_ref=src, dst_ref=dst, send_sem=send, recv_sem=recv, device_id=to, device_id_type=MESH)

    def swap(c, j):
        return remote(swap_out.at[j], swap_in.at[c % 2, j], swap_ss.at[j], swap_rs.at[c % 2, j], partner)

    def rs1(c, d):
        return remote(rs1_out.at[d], rs1_in.at[c % 2, d], rs1_ss.at[d], rs1_rs.at[c % 2, d], beside[d])

    def rs2(c, d, part):
        return remote(
            rs2_out.at[d, part_rows(part)], rs2_in.at[c % 2, d, part_rows(part)], rs2_ss.at[d, part], rs2_rs.at[c % 2, d, part], beside[d]
        )

    def ag1(c, d, part):
        there = y_hbm.at[rows_of(c, part), columns(chip, core)]
        return remote(fin_s.at[part_rows(part)], there, ag1_ss.at[d, part], ag1_rs.at[c % 2, d, part], beside[d])

    def ag2(c, d):
        there = y_hbm.at[rows_of(c, d), columns(places[FROM[d]], core)]
        return remote(there, there, ag2_ss.at[d], ag2_rs.at[c % 2, d], beside[d])

    def pair(c, j):
        there = y_hbm.at[rows_of(c), columns(places[j], core)]
        return remote(fin_s if j == SELF else there, there, pair_ss.at[j], pair_rs.at[c % 2, j], partner)

    def put(c):
        return pltpu.make_async_copy(fin_s, y_hbm.at[rows_of(c), columns(chip, core)], put_sem)

    def put_last():
        return pltpu.make_async_copy(fin_s, fin_hbm, put_sem)

    def residual(c):
        return pltpu.make_async_copy(x_hbm.at[rows_of(c), columns(chip, core)], res_s.at[c % 2], res_sem.at[c % 2])

    def load_x(c, part):
        rows_here = pl.ds(pl.multiple_of(c * chunk + part * (chunk // X_PARTS), chunk // X_PARTS), chunk // X_PARTS)
        return pltpu.make_async_copy(x_hbm.at[rows_here], x_s.at[pl.ds(part * (chunk // X_PARTS), chunk // X_PARTS)], x_sem.at[part])

    def weight(i, n, slot):
        rows_here = pl.ds(pl.multiple_of(i * kb, kb), kb)
        there = w_s.at[slot, pl.ds(0, kb), pl.ds(n * wide, wide)]
        return pltpu.make_async_copy((wq_hbm, wk_hbm, wv_hbm)[n].at[rows_here], there, w_sem.at[slot, n])

    def out_weight(p, n, slot):
        j = p * 2 + n
        place = (chip + 2 + j) % chips
        whose = jnp.where(j < chips, 1 - core, core)
        there = w_s.at[slot, pl.ds(0, wide), pl.ds(n * piece, piece)]
        return pltpu.make_async_copy(wo_hbm.at[:, columns(place, whose)], there, w_sem.at[slot, n])

    def slot_of(c, t):
        return (c * tiles + t) % SLOTS

    def fetch(c, t):
        slot = slot_of(c, t)
        later = t >= tiles
        t = jnp.where(later, t - tiles, t)
        live = jnp.where(later, c + 1, c) < chunks

        @pl.when(live & (t < blocks))
        def _():
            for n in range(3):
                weight(t, n, slot).start()

        @pl.when(live & (t >= blocks))
        def _():
            for n in range(2):
                out_weight(t - blocks, n, slot).start()

    def strips(count, body):
        lax.fori_loop(0, count // STRIP, lambda r, _: body(pl.ds(pl.multiple_of(r * STRIP, STRIP), STRIP)), None)

    def strips_of(part, body):
        lax.fori_loop(
            0,
            half // STRIP,
            lambda r, _: body(pl.ds(pl.multiple_of(part * half + r * STRIP, STRIP), STRIP), pl.ds(pl.multiple_of(r * STRIP, STRIP), STRIP)),
            None,
        )

    def norm(c):
        def body(r):
            total = jnp.zeros((STRIP, kb), F32)
            for i in range(blocks):
                part = x_s[r, i * kb : (i + 1) * kb].astype(F32)
                total += part * part
            scale = lax.rsqrt(jnp.sum(total, axis=-1, keepdims=True) / depth + 1e-6)
            for i in range(blocks):
                part = x_s[r, i * kb : (i + 1) * kb].astype(F32)
                a_s[i, r, :] = (part * scale * gain_s[:, i * kb : (i + 1) * kb]).astype(BF16)

        each = chunk // X_PARTS // STRIP
        for part in range(X_PARTS):
            load_x(c, part).wait()
            lax.fori_loop(part * each, (part + 1) * each, lambda r, _: body(pl.ds(pl.multiple_of(r * STRIP, STRIP), STRIP)), None)

        @pl.when(c + 1 < chunks)
        def _():
            for part in range(X_PARTS):
                load_x(c + 1, part).start()

    def project(c, first, last):
        def product(i):
            slot = slot_of(c, i)
            for n in range(3):
                weight(i, n, slot).wait()
            fetch(c, i + SLOTS - 1)
            return _dot(a_s[i], w_s[slot, :kb, : 3 * wide], 1, 0)

        def body(i, _):
            acc_s[...] += product(i)

        if first == 0:
            acc_s[...] = product(0)
        lax.fori_loop(max(first, 1), last, body, None)

    def turn(c, ref, at, n):
        ca, sa = ca_ref[pl.ds(c, 1), :], sa_ref[pl.ds(c, 1), :]

        def body(r):
            cb, sb = cb_ref[r, :], sb_ref[r, :]
            cos, sin = ca * cb - sa * sb, sa * cb + ca * sb
            for h in range(heads):
                t = acc_s[r, n * wide + h * HEAD : n * wide + (h + 1) * HEAD].astype(BF16).astype(F32)
                turned = t * cos + pltpu.roll(t, HEAD // 2, 1) * sin
                ref[h, pl.ds(pl.multiple_of(at + r.start, STRIP), STRIP), :] = turned.astype(BF16)

        strips(chunk, body)

    def keep_values(c):
        for h in range(heads):
            vt_s[h, :HEAD, rows_of(c)] = acc_s[:, 2 * wide + h * HEAD : 2 * wide + (h + 1) * HEAD].astype(BF16).T

    def attend(c):
        top_s[...] = jnp.full(top_s.shape, NEG, F32)
        mix_s[...] = jnp.zeros(mix_s.shape, F32)

        def block(j, masked):
            here = rows_of(j)
            scores = [_dot(k_s[h, here, :], q_s[h], 1, 1) for h in range(heads)]
            if masked:
                ok = lax.broadcasted_iota(jnp.int32, (chunk, chunk), 1) >= lax.broadcasted_iota(jnp.int32, (chunk, chunk), 0)
            weights, keeps = [], []
            for h, s in enumerate(scores):
                if masked:
                    s = jnp.where(ok, s, HIDDEN)
                old = top_s[h : h + 1, :]
                top = jnp.maximum(old, s.max(axis=0, keepdims=True))
                top_s[h : h + 1, :] = top
                weights.append(jnp.exp2((s - top) * e).astype(BF16))
                keeps.append(jnp.exp2((old - top) * e))
            for h in range(heads):
                mix_s[h] = mix_s[h] * keeps[h] + _dot(vt_s[h, :, here], weights[h], 1, 0)

        lax.fori_loop(0, c, lambda j, _: block(j, False), None)
        block(c, True)
        for h in range(heads):
            out = mix_s[h, :HEAD, :] * (1 / mix_s[h, HEAD : HEAD + 1, :])
            seen_s[:, h * HEAD : (h + 1) * HEAD] = out.T.astype(BF16)

    def project_out(c):
        for p in range(chips):
            if p == chips - 1:
                scatter_opposite(c)
            slot = slot_of(c, blocks + p)
            for n in range(2):
                out_weight(p, n, slot).wait()
            fetch(c, blocks + p + SLOTS - 1)
            product = _dot(seen_s[...], w_s[slot, :wide, : 2 * piece], 1, 0)
            for n in range(2):
                j = p * 2 + n
                part = product[:, n * piece : (n + 1) * piece]
                if j < chips:

                    @pl.when(c > 0)
                    def _():
                        swap(c - 1, j).wait_send()

                    swap_out[j] = part.astype(BF16)
                else:
                    own_s[c % 2, j - chips] = part
            if 1 <= p <= chips // 2:
                for n in range(2):
                    swap(c, p * 2 - 2 + n).start()

    def chip_sum(c, j, r):
        return own_s[c % 2, j, r, :] + swap_in[c % 2, j, r, :].astype(F32)

    def scatter_opposite(c):
        residual(c).start()
        swap(c, OPP).wait_recv()

        @pl.when(c > 0)
        def _():
            for d in range(2):
                rs1(c - 1, d).wait_send()

        for d in range(2):

            def body(r, to):
                rs1_out[d, to, :] = chip_sum(c, OPP, r).astype(BF16)

            strips_of(d, body)
        for d in range(2):
            rs1(c, d).start()

    def scatter(c):
        for j in (LEFT, SELF, RIGHT):
            swap(c, j).wait_recv()

        @pl.when(c > 0)
        def _():
            for d in range(2):
                rs2(c - 1, d, 1 - d).wait_send()

        for d in range(2):

            def body(r, to):
                rs2_out[d, r, :] = chip_sum(c, TOWARDS[d], r).astype(BF16)

            strips_of(1 - d, body)
        for d in range(2):
            rs2(c, d, 1 - d).start()

    def add_on(c):
        for d in range(2):
            rs1(c, d).wait_recv()

            @pl.when(c > 0)
            def _():
                rs2(c - 1, d, d).wait_send()

            def body(r, to):
                rs2_out[d, r, :] = (chip_sum(c, TOWARDS[d], r) + rs1_in[c % 2, d, to, :].astype(F32)).astype(BF16)

            strips_of(d, body)
        for d in range(2):
            rs2(c, d, d).start()

    def finish(c):
        residual(c).wait()
        for d in range(2):
            for part in range(2):
                rs2(c, d, part).wait_recv()

        @pl.when(c > 0)
        def _():
            for d in range(2):
                for part in range(2):
                    ag1(c - 1, d, part).wait_send()
            pair(c - 1, SELF).wait_send()
            put(c - 1).wait()

        def body(r):
            total = chip_sum(c, SELF, r)
            for d in range(2):
                total += rs2_in[c % 2, d, r, :].astype(F32)
            fin_s[r, :] = (total + res_s[c % 2, r, :].astype(F32)).astype(BF16)

        strips(chunk, body)

        @pl.when(c < chunks - 1)
        def _():
            for other in range(2):
                for d in range(2):
                    ag1(c, d, d if other == 0 else 1 - d).start()
            pair(c, SELF).start()
            put(c).start()

        @pl.when(c == chunks - 1)
        def _():
            put_last().start()

    def pass_on(c):
        for d in range(2):
            ag1(c, d, d).wait_recv()

            @pl.when(c > 0)
            def _():
                ag2(c - 1, d).wait_send()

            ag2(c, d).start()

    def give_partner(c):
        for d in range(2):
            ag1(c, d, 1 - d).wait_recv()

            @pl.when(c > 0)
            def _():
                pair(c - 1, FROM[d]).wait_send()

            pair(c, FROM[d]).start()
        for d in range(2):
            ag2(c, d).wait_recv()

        @pl.when(c > 0)
        def _():
            pair(c - 1, OPP).wait_send()

        pair(c, OPP).start()

    barrier = pltpu.get_barrier_semaphore()
    for part in range(X_PARTS):
        load_x(0, part).start()
    for t in range(SLOTS - 1):
        fetch(0, t)
    for to in (*beside, partner):
        pl.semaphore_signal(barrier, inc=1, device_id=to, device_id_type=MESH)
    for h in range(heads):
        vt_s[h, HEAD:, :] = jnp.ones((ONES, rows), BF16)
    for i in range(blocks):
        gain_s[:, i * kb : (i + 1) * kb] = gain_ref[pl.ds(i * kb, kb)].astype(F32).reshape(1, kb)
    pl.semaphore_wait(barrier, 3)

    def step(c, _):
        new = c < chunks
        last = (c >= 1) & (c <= chunks)
        before = c >= 2
        early = blocks // 2

        @pl.when(new)
        def _():
            norm(c)
            project(c, 0, early)

        @pl.when(last)
        def _():
            add_on(c - 1)

        @pl.when(before)
        def _():
            pass_on(c - 2)

        @pl.when(c >= 3)
        def _():
            for j in (LEFT, RIGHT, OPP):
                pair(c - 3, j).wait_recv()

        @pl.when(new)
        def _():
            project(c, early, blocks)
            turn(c, q_s, 0, 0)
            turn(c, k_s, c * chunk, 1)
            keep_values(c)

        @pl.when(last)
        def _():
            finish(c - 1)

        @pl.when(new)
        def _():
            attend(c)

        @pl.when(before)
        def _():
            pair(c - 2, SELF).wait_recv()

        @pl.when(new)
        def _():
            project_out(c)
            scatter(c)

        @pl.when(before)
        def _():
            give_partner(c - 2)

    lax.fori_loop(0, chunks + 1, step, None)

    c = chunks - 1
    for j in range(chips):
        swap(c, j).wait_send()
    for d in range(2):
        rs1(c, d).wait_send()
        ag2(c - 1, d).wait_send()
        for part in range(2):
            rs2(c, d, part).wait_send()
    put_last().wait()
    for j in (LEFT, RIGHT, OPP):
        pair(c - 1, j).wait_send()
        pair(c - 1, j).wait_recv()


def _copy_kernel(first, count, *refs):
    src, dst, buf, in_sem, out_sem = refs[0], refs[-4], *refs[-3:]
    slots, each = buf.shape[:2]

    def take(i):
        return pltpu.make_async_copy(src.at[pl.ds((first + i) * each, each)], buf.at[i % slots], in_sem.at[i % slots])

    def give(i):
        return pltpu.make_async_copy(buf.at[i % slots], dst.at[pl.ds((first + i) * each, each)], out_sem.at[i % slots])

    ahead = slots // 2
    for i in range(min(ahead, count)):
        take(i).start()
    for i in range(count):
        take(i).wait()
        give(i).start()
        if i + ahead < count:
            if i + ahead >= slots:
                give(i + ahead - slots).wait()
            take(i + ahead).start()
    for i in range(max(count - slots, 0), count):
        give(i).wait()


def _copy_rows(src, first, count, each, into=None):
    hbm = pl.BlockSpec(memory_space=pl.ANY)
    given = (src,) if into is None else (src, into)
    slots = 16
    return pl.pallas_call(
        functools.partial(_copy_kernel, first, count),
        out_shape=jax.ShapeDtypeStruct(src.shape, src.dtype),
        in_specs=[hbm] * len(given),
        out_specs=hbm,
        scratch_shapes=[
            pltpu.VMEM((slots, each, src.shape[1]), src.dtype), pltpu.SemaphoreType.DMA((slots,)), pltpu.SemaphoreType.DMA((slots,)),
        ],
        input_output_aliases={} if into is None else {1: 0},
        compiler_params=pltpu.CompilerParams(vmem_limit_bytes=40 * 2**20),
        cost_estimate=pl.CostEstimate(flops=count * each * src.shape[1] * 200, bytes_accessed=count * each * src.shape[1] * 4, transcendentals=0),
    )(*given)


def _place_kernel(group, kinds, _, *refs):
    pieces, out, sem = refs[:-2], refs[-2], refs[-1]
    me = lax.axis_index("tp")
    chips = group // 2
    chip, core = me // 2, me % 2
    places = [(chip + by) % chips for by in (2, 2, chips - 1, 0, 1)]
    rows = out.shape[0]
    chunk, piece = 2 * min(ref.shape[0] for ref in pieces), pieces[0].shape[1]
    copies = []
    for n, (kind, ref) in enumerate(zip(kinds, pieces)):
        j = kind % 5
        at = rows - chunk + (chunk // 2 if j == 1 else 0)
        whose = core if kind < 5 else 1 - core
        columns = pl.ds(pl.multiple_of((places[j] * 2 + whose) * piece, piece), piece)
        copies.append(pltpu.make_async_copy(ref, out.at[pl.ds(at, ref.shape[0]), columns], sem.at[n]))
    for copy in copies:
        copy.start()
    for copy in copies:
        copy.wait()


def _place(group, y, kinds, pieces):
    hbm, vmem = pl.BlockSpec(memory_space=pl.ANY), pl.BlockSpec(memory_space=pltpu.VMEM)
    return pl.pallas_call(
        functools.partial(_place_kernel, group, kinds),
        out_shape=jax.ShapeDtypeStruct(y.shape, y.dtype),
        in_specs=[hbm] + [vmem] * len(pieces),
        out_specs=hbm,
        scratch_shapes=[pltpu.SemaphoreType.DMA((len(pieces),))],
        input_output_aliases={0: 0},
        compiler_params=pltpu.CompilerParams(vmem_limit_bytes=16 * 2**20),
        cost_estimate=pl.CostEstimate(flops=10**6, bytes_accessed=10**7, transcendentals=0),
    )(y, *pieces)


def _tables(rows, chunk):
    half = HEAD // 2
    rate = float(THETA) ** (-np.arange(half) / half)

    def pairs(place):
        angle = place[:, None] * rate
        cos, sin = np.cos(angle), np.sin(angle)
        return np.concatenate([cos, cos], -1).astype(np.float32), np.concatenate([-sin, sin], -1).astype(np.float32)

    return *pairs(np.arange(chunk)), *pairs(np.arange(0, rows, chunk))


def solution(mesh):
    group = mesh.shape["tp"]

    def step(x, gain, wq, wk, wv, wo):
        rows, depth = x.shape
        wide = wq.shape[1]
        heads, piece = wide // HEAD, depth // group
        chunk = ROWS
        chunks, half = rows // chunk, chunk // 2
        kb = _fit(depth, BLOCK)
        blocks = depth // kb
        tables = _tables(rows, chunk)
        vmem, hbm = pl.BlockSpec(memory_space=pltpu.VMEM), pl.BlockSpec(memory_space=pl.ANY)
        dma = lambda *shape: pltpu.SemaphoreType.DMA(shape)
        early, done = pl.pallas_call(
            functools.partial(_kernel, group),
            out_shape=[jax.ShapeDtypeStruct((rows, depth), BF16), jax.ShapeDtypeStruct((chunk, piece), BF16)],
            in_specs=[hbm, vmem, hbm, hbm, hbm, hbm, vmem, vmem, vmem, vmem],
            out_specs=[hbm, hbm],
            scratch_shapes=[
                pltpu.VMEM((chunk, depth), BF16),
                pltpu.VMEM((blocks, chunk, kb), BF16),
                pltpu.VMEM((SLOTS, max(kb, wide), max(3 * wide, 2 * piece)), BF16),
                pltpu.VMEM((chunk, 3 * wide), F32),
                pltpu.VMEM((heads, chunk, HEAD), BF16),
                pltpu.VMEM((heads, rows, HEAD), BF16),
                pltpu.VMEM((heads, HEAD + ONES, rows), BF16),
                pltpu.VMEM((heads, chunk), F32),
                pltpu.VMEM((heads, HEAD + ONES, chunk), F32),
                pltpu.VMEM((chunk, wide), BF16),
                pltpu.VMEM((2, group // 2, chunk, piece), F32),
                pltpu.VMEM((group // 2, chunk, piece), BF16),
                pltpu.VMEM((2, group // 2, chunk, piece), BF16),
                pltpu.VMEM((2, half, piece), BF16),
                pltpu.VMEM((2, 2, half, piece), BF16),
                pltpu.VMEM((2, chunk, piece), BF16),
                pltpu.VMEM((2, 2, chunk, piece), BF16),
                pltpu.VMEM((chunk, piece), BF16),
                pltpu.VMEM((2, chunk, piece), BF16),
                pltpu.VMEM((1, depth), F32),
                dma(SLOTS, 3), dma(X_PARTS), dma(2),
                dma(group // 2), dma(2, group // 2),
                dma(2), dma(2, 2),
                dma(2, 2), dma(2, 2, 2),
                dma(2, 2), dma(2, 2, 2),
                dma(2), dma(2, 2),
                dma(group // 2), dma(2, group // 2),
                pltpu.SemaphoreType.DMA,
            ],
            compiler_params=pltpu.CompilerParams(collective_id=0, has_side_effects=True, vmem_limit_bytes=62 * 2**20),
        )(x, gain, wq, wk, wv, wo, *tables)

        right = [(i, (i + 2) % group) for i in range(group)]
        left = [(i, (i - 2) % group) for i in range(group)]
        other = [(i, i + 1 - 2 * (i % 2)) for i in range(group)]
        send = lambda t, to: lax.ppermute(t, "tp", to)
        from_left, from_right, theirs = send(done, right), send(done, left), send(done, other)
        each = chunk // 4
        count = (chunks - 1) * 4
        y = _copy_rows(early, 0, SPLIT, each)
        y, from_left, from_right = lax.optimization_barrier((y, from_left, from_right))
        opp_a, opp_b = send(from_left[:half], right), send(from_right[half:], left)
        sides = send(from_left, other), send(from_right, other)
        y = _copy_rows(early, SPLIT, count - SPLIT, each, y)
        y, opp_a, opp_b = lax.optimization_barrier((y, opp_a, opp_b))
        given = send(opp_a, other), send(opp_b, other)
        y = _place(group, y, (0, 1, 2, 3, 4, 7, 8, 9), (opp_a, opp_b, from_left, done, from_right, sides[0], theirs, sides[1]))
        return _place(group, y, (5, 6), given)

    tokens, columns = P("dp", None), P(None, "tp")
    return jax.shard_map(
        step,
        mesh=mesh,
        in_specs=(tokens, P(None), columns, columns, columns, P("tp", None)),
        out_specs=tokens,
        check_vma=False,
    )
```

```python
import functools

import jax
import jax.numpy as jnp
import numpy as np
from jax import lax
from jax.experimental import pallas as pl
from jax.experimental.pallas import tpu as pltpu
from jax.sharding import PartitionSpec as P

HEAD = 128
THETA = 10000
ROWS = 256
BLOCK = 1024
SLOTS = 3
X_PARTS = 4
STRIP = 32
SPLIT = 24
ONES = 16
NEG = -1e30
HIDDEN = 2 * NEG
LOG2E = 1.4426950408889634
OPP, LEFT, SELF, RIGHT = range(4)
TOWARDS = (RIGHT, LEFT)
FROM = (LEFT, RIGHT)
MESH = pl.DeviceIdType.MESH
F32, BF16 = jnp.float32, jnp.bfloat16


def _fit(size, want, unit=128):
    return max(n for n in range(unit, want + 1, unit) if size % n == 0)


def _dot(a, b, ca, cb):
    return lax.dot_general(a, b, (((ca,), (cb,)), ((), ())), preferred_element_type=F32)


def _kernel(
    group, x_hbm, gain_ref, wq_hbm, wk_hbm, wv_hbm, wo_hbm, cb_ref, sb_ref, ca_ref, sa_ref, y_hbm, fin_hbm,
    x_s, a_s, w_s, acc_s, q_s, k_s, vt_s, top_s, mix_s, seen_s, own_s, swap_out, swap_in, rs1_out, rs1_in, rs2_out, rs2_in, fin_s, res_s, gain_s,
    w_sem, x_sem, res_sem, swap_ss, swap_rs, rs1_ss, rs1_rs, rs2_ss, rs2_rs, ag1_ss, ag1_rs, ag2_ss, ag2_rs, pair_ss, pair_rs, put_sem,
):
    rows, depth = x_hbm.shape
    wide = wq_hbm.shape[1]
    piece = depth // group
    heads = wide // HEAD
    chunk = x_s.shape[0]
    chunks = rows // chunk
    half = chunk // 2
    blocks, _, kb = a_s.shape
    tiles = blocks + group // 2
    e = HEAD**-0.5 * LOG2E

    me = lax.axis_index("tp")
    chips = group // 2
    chip, core = me // 2, me % 2
    places = [(chip + by) % chips for by in (2, chips - 1, 0, 1)]
    partner = {"tp": chip * 2 + 1 - core}
    beside = [{"tp": places[TOWARDS[d]] * 2 + core} for d in range(2)]

    def columns(place, whose):
        return pl.ds(pl.multiple_of((place * 2 + whose) * piece, piece), piece)

    def rows_of(c, part=None):
        if part is None:
            return pl.ds(pl.multiple_of(c * chunk, chunk), chunk)
        return pl.ds(pl.multiple_of(c * chunk + part * half, half), half)

    def part_rows(part):
        return pl.ds(part * half, half)

    def remote(src, dst, send, recv, to):
        return pltpu.make_async_remote_copy(src_ref=src, dst_ref=dst, send_sem=send, recv_sem=recv, device_id=to, device_id_type=MESH)

    def swap(c, j):
        return remote(swap_out.at[j], swap_in.at[c % 2, j], swap_ss.at[j], swap_rs.at[c % 2, j], partner)

    def rs1(c, d):
        return remote(rs1_out.at[d], rs1_in.at[c % 2, d], rs1_ss.at[d], rs1_rs.at[c % 2, d], beside[d])

    def rs2(c, d, part):
        return remote(
            rs2_out.at[d, part_rows(part)], rs2_in.at[c % 2, d, part_rows(part)], rs2_ss.at[d, part], rs2_rs.at[c % 2, d, part], beside[d]
        )

    def ag1(c, d, part):
        there = y_hbm.at[rows_of(c, part), columns(chip, core)]
        return remote(fin_s.at[part_rows(part)], there, ag1_ss.at[d, part], ag1_rs.at[c % 2, d, part], beside[d])

    def ag2(c, d):
        there = y_hbm.at[rows_of(c, d), columns(places[FROM[d]], core)]
        return remote(there, there, ag2_ss.at[d], ag2_rs.at[c % 2, d], beside[d])

    def pair(c, j):
        there = y_hbm.at[rows_of(c), columns(places[j], core)]
        return remote(fin_s if j == SELF else there, there, pair_ss.at[j], pair_rs.at[c % 2, j], partner)

    def put(c):
        return pltpu.make_async_copy(fin_s, y_hbm.at[rows_of(c), columns(chip, core)], put_sem)

    def put_last():
        return pltpu.make_async_copy(fin_s, fin_hbm, put_sem)

    def residual(c):
        return pltpu.make_async_copy(x_hbm.at[rows_of(c), columns(chip, core)], res_s.at[c % 2], res_sem.at[c % 2])

    def load_x(c, part):
        rows_here = pl.ds(pl.multiple_of(c * chunk + part * (chunk // X_PARTS), chunk // X_PARTS), chunk // X_PARTS)
        return pltpu.make_async_copy(x_hbm.at[rows_here], x_s.at[pl.ds(part * (chunk // X_PARTS), chunk // X_PARTS)], x_sem.at[part])

    def weight(i, n, slot):
        rows_here = pl.ds(pl.multiple_of(i * kb, kb), kb)
        there = w_s.at[slot, pl.ds(0, kb), pl.ds(n * wide, wide)]
        return pltpu.make_async_copy((wq_hbm, wk_hbm, wv_hbm)[n].at[rows_here], there, w_sem.at[slot, n])

    def out_weight(p, n, slot):
        j = p * 2 + n
        place = (chip + 2 + j) % chips
        whose = jnp.where(j < chips, 1 - core, core)
        there = w_s.at[slot, pl.ds(0, wide), pl.ds(n * piece, piece)]
        return pltpu.make_async_copy(wo_hbm.at[:, columns(place, whose)], there, w_sem.at[slot, n])

    def slot_of(c, t):
        return (c * tiles + t) % SLOTS

    def fetch(c, t):
        slot = slot_of(c, t)
        later = t >= tiles
        t = jnp.where(later, t - tiles, t)
        live = jnp.where(later, c + 1, c) < chunks

        @pl.when(live & (t < blocks))
        def _():
            for n in range(3):
                weight(t, n, slot).start()

        @pl.when(live & (t >= blocks))
        def _():
            for n in range(2):
                out_weight(t - blocks, n, slot).start()

    def strips(count, body):
        lax.fori_loop(0, count // STRIP, lambda r, _: body(pl.ds(pl.multiple_of(r * STRIP, STRIP), STRIP)), None)

    def strips_of(part, body):
        lax.fori_loop(
            0,
            half // STRIP,
            lambda r, _: body(pl.ds(pl.multiple_of(part * half + r * STRIP, STRIP), STRIP), pl.ds(pl.multiple_of(r * STRIP, STRIP), STRIP)),
            None,
        )

    def norm(c):
        def body(r):
            total = jnp.zeros((STRIP, kb), F32)
            for i in range(blocks):
                part = x_s[r, i * kb : (i + 1) * kb].astype(F32)
                total += part * part
            scale = lax.rsqrt(jnp.sum(total, axis=-1, keepdims=True) / depth + 1e-6)
            for i in range(blocks):
                part = x_s[r, i * kb : (i + 1) * kb].astype(F32)
                a_s[i, r, :] = (part * scale * gain_s[:, i * kb : (i + 1) * kb]).astype(BF16)

        each = chunk // X_PARTS // STRIP
        for part in range(X_PARTS):
            load_x(c, part).wait()
            lax.fori_loop(part * each, (part + 1) * each, lambda r, _: body(pl.ds(pl.multiple_of(r * STRIP, STRIP), STRIP)), None)

        @pl.when(c + 1 < chunks)
        def _():
            for part in range(X_PARTS):
                load_x(c + 1, part).start()

    def project(c, first, last):
        def product(i):
            slot = slot_of(c, i)
            for n in range(3):
                weight(i, n, slot).wait()
            fetch(c, i + SLOTS - 1)
            return _dot(a_s[i], w_s[slot, :kb, : 3 * wide], 1, 0)

        def body(i, _):
            acc_s[...] += product(i)

        if first == 0:
            acc_s[...] = product(0)
        lax.fori_loop(max(first, 1), last, body, None)

    def turn(c, ref, at, n):
        ca, sa = ca_ref[pl.ds(c, 1), :], sa_ref[pl.ds(c, 1), :]

        def body(r):
            cb, sb = cb_ref[r, :], sb_ref[r, :]
            cos, sin = ca * cb - sa * sb, sa * cb + ca * sb
            for h in range(heads):
                t = acc_s[r, n * wide + h * HEAD : n * wide + (h + 1) * HEAD].astype(BF16).astype(F32)
                turned = t * cos + pltpu.roll(t, HEAD // 2, 1) * sin
                ref[h, pl.ds(pl.multiple_of(at + r.start, STRIP), STRIP), :] = turned.astype(BF16)

        strips(chunk, body)

    def keep_values(c):
        for h in range(heads):
            vt_s[h, :HEAD, rows_of(c)] = acc_s[:, 2 * wide + h * HEAD : 2 * wide + (h + 1) * HEAD].astype(BF16).T

    def attend(c):
        top_s[...] = jnp.full(top_s.shape, NEG, F32)
        mix_s[...] = jnp.zeros(mix_s.shape, F32)

        def block(j, masked):
            here = rows_of(j)
            scores = [_dot(k_s[h, here, :], q_s[h], 1, 1) for h in range(heads)]
            if masked:
                ok = lax.broadcasted_iota(jnp.int32, (chunk, chunk), 1) >= lax.broadcasted_iota(jnp.int32, (chunk, chunk), 0)
            weights, keeps = [], []
            for h, s in enumerate(scores):
                if masked:
                    s = jnp.where(ok, s, HIDDEN)
                old = top_s[h : h + 1, :]
                top = jnp.maximum(old, s.max(axis=0, keepdims=True))
                top_s[h : h + 1, :] = top
                weights.append(jnp.exp2((s - top) * e).astype(BF16))
                keeps.append(jnp.exp2((old - top) * e))
            for h in range(heads):
                mix_s[h] = mix_s[h] * keeps[h] + _dot(vt_s[h, :, here], weights[h], 1, 0)

        lax.fori_loop(0, c, lambda j, _: block(j, False), None)
        block(c, True)
        for h in range(heads):
            out = mix_s[h, :HEAD, :] * (1 / mix_s[h, HEAD : HEAD + 1, :])
            seen_s[:, h * HEAD : (h + 1) * HEAD] = out.T.astype(BF16)

    def project_out(c):
        for p in range(chips):
            if p == chips - 1:
                scatter_opposite(c)
            slot = slot_of(c, blocks + p)
            for n in range(2):
                out_weight(p, n, slot).wait()
            fetch(c, blocks + p + SLOTS - 1)
            product = _dot(seen_s[...], w_s[slot, :wide, : 2 * piece], 1, 0)
            for n in range(2):
                j = p * 2 + n
                part = product[:, n * piece : (n + 1) * piece]
                if j < chips:

                    @pl.when(c > 0)
                    def _():
                        swap(c - 1, j).wait_send()

                    swap_out[j] = part.astype(BF16)
                else:
                    own_s[c % 2, j - chips] = part
            if 1 <= p <= chips // 2:
                for n in range(2):
                    swap(c, p * 2 - 2 + n).start()

    def chip_sum(c, j, r):
        return own_s[c % 2, j, r, :] + swap_in[c % 2, j, r, :].astype(F32)

    def scatter_opposite(c):
        residual(c).start()
        swap(c, OPP).wait_recv()

        @pl.when(c > 0)
        def _():
            for d in range(2):
                rs1(c - 1, d).wait_send()

        for d in range(2):

            def body(r, to):
                rs1_out[d, to, :] = chip_sum(c, OPP, r).astype(BF16)

            strips_of(d, body)
        for d in range(2):
            rs1(c, d).start()

    def scatter(c):
        for j in (LEFT, SELF, RIGHT):
            swap(c, j).wait_recv()

        @pl.when(c > 0)
        def _():
            for d in range(2):
                rs2(c - 1, d, 1 - d).wait_send()

        for d in range(2):

            def body(r, to):
                rs2_out[d, r, :] = chip_sum(c, TOWARDS[d], r).astype(BF16)

            strips_of(1 - d, body)
        for d in range(2):
            rs2(c, d, 1 - d).start()

    def add_on(c):
        for d in range(2):
            rs1(c, d).wait_recv()

            @pl.when(c > 0)
            def _():
                rs2(c - 1, d, d).wait_send()

            def body(r, to):
                rs2_out[d, r, :] = (chip_sum(c, TOWARDS[d], r) + rs1_in[c % 2, d, to, :].astype(F32)).astype(BF16)

            strips_of(d, body)
        for d in range(2):
            rs2(c, d, d).start()

    def finish(c):
        residual(c).wait()
        for d in range(2):
            for part in range(2):
                rs2(c, d, part).wait_recv()

        @pl.when(c > 0)
        def _():
            for d in range(2):
                for part in range(2):
                    ag1(c - 1, d, part).wait_send()
            pair(c - 1, SELF).wait_send()
            put(c - 1).wait()

        def body(r):
            total = chip_sum(c, SELF, r)
            for d in range(2):
                total += rs2_in[c % 2, d, r, :].astype(F32)
            fin_s[r, :] = (total + res_s[c % 2, r, :].astype(F32)).astype(BF16)

        strips(chunk, body)

        @pl.when(c < chunks - 1)
        def _():
            for other in range(2):
                for d in range(2):
                    ag1(c, d, d if other == 0 else 1 - d).start()
            pair(c, SELF).start()
            put(c).start()

        @pl.when(c == chunks - 1)
        def _():
            put_last().start()

    def pass_on(c):
        for d in range(2):
            ag1(c, d, d).wait_recv()

            @pl.when(c > 0)
            def _():
                ag2(c - 1, d).wait_send()

            ag2(c, d).start()

    def give_partner(c):
        for d in range(2):
            ag1(c, d, 1 - d).wait_recv()

            @pl.when(c > 0)
            def _():
                pair(c - 1, FROM[d]).wait_send()

            pair(c, FROM[d]).start()
        for d in range(2):
            ag2(c, d).wait_recv()

        @pl.when(c > 0)
        def _():
            pair(c - 1, OPP).wait_send()

        pair(c, OPP).start()

    barrier = pltpu.get_barrier_semaphore()
    for part in range(X_PARTS):
        load_x(0, part).start()
    for t in range(SLOTS - 1):
        fetch(0, t)
    for to in (*beside, partner):
        pl.semaphore_signal(barrier, inc=1, device_id=to, device_id_type=MESH)
    for h in range(heads):
        vt_s[h, HEAD:, :] = jnp.ones((ONES, rows), BF16)
    for i in range(blocks):
        gain_s[:, i * kb : (i + 1) * kb] = gain_ref[pl.ds(i * kb, kb)].astype(F32).reshape(1, kb)
    pl.semaphore_wait(barrier, 3)

    def step(c, _):
        new = c < chunks
        last = (c >= 1) & (c <= chunks)
        before = c >= 2
        early = blocks // 2

        @pl.when(new)
        def _():
            norm(c)
            project(c, 0, early)

        @pl.when(last)
        def _():
            add_on(c - 1)

        @pl.when(before)
        def _():
            pass_on(c - 2)

        @pl.when(c >= 3)
        def _():
            for j in (LEFT, RIGHT, OPP):
                pair(c - 3, j).wait_recv()

        @pl.when(new)
        def _():
            project(c, early, blocks)
            turn(c, q_s, 0, 0)
            turn(c, k_s, c * chunk, 1)
            keep_values(c)

        @pl.when(last)
        def _():
            finish(c - 1)

        @pl.when(new)
        def _():
            attend(c)

        @pl.when(before)
        def _():
            pair(c - 2, SELF).wait_recv()

        @pl.when(new)
        def _():
            project_out(c)
            scatter(c)

        @pl.when(before)
        def _():
            give_partner(c - 2)

    lax.fori_loop(0, chunks + 1, step, None)

    c = chunks - 1
    for j in range(chips):
        swap(c, j).wait_send()
    for d in range(2):
        rs1(c, d).wait_send()
        ag2(c - 1, d).wait_send()
        for part in range(2):
            rs2(c, d, part).wait_send()
    put_last().wait()
    for j in (LEFT, RIGHT, OPP):
        pair(c - 1, j).wait_send()
        pair(c - 1, j).wait_recv()


def _copy_kernel(first, count, *refs):
    src, dst, buf, in_sem, out_sem = refs[0], refs[-4], *refs[-3:]
    slots, each = buf.shape[:2]

    def take(i):
        return pltpu.make_async_copy(src.at[pl.ds((first + i) * each, each)], buf.at[i % slots], in_sem.at[i % slots])

    def give(i):
        return pltpu.make_async_copy(buf.at[i % slots], dst.at[pl.ds((first + i) * each, each)], out_sem.at[i % slots])

    ahead = slots // 2
    for i in range(min(ahead, count)):
        take(i).start()
    for i in range(count):
        take(i).wait()
        give(i).start()
        if i + ahead < count:
            if i + ahead >= slots:
                give(i + ahead - slots).wait()
            take(i + ahead).start()
    for i in range(max(count - slots, 0), count):
        give(i).wait()


def _copy_rows(src, first, count, each, into=None):
    hbm = pl.BlockSpec(memory_space=pl.ANY)
    given = (src,) if into is None else (src, into)
    slots = 16
    return pl.pallas_call(
        functools.partial(_copy_kernel, first, count),
        out_shape=jax.ShapeDtypeStruct(src.shape, src.dtype),
        in_specs=[hbm] * len(given),
        out_specs=hbm,
        scratch_shapes=[
            pltpu.VMEM((slots, each, src.shape[1]), src.dtype), pltpu.SemaphoreType.DMA((slots,)), pltpu.SemaphoreType.DMA((slots,)),
        ],
        input_output_aliases={} if into is None else {1: 0},
        compiler_params=pltpu.CompilerParams(vmem_limit_bytes=40 * 2**20),
        cost_estimate=pl.CostEstimate(flops=count * each * src.shape[1] * 200, bytes_accessed=count * each * src.shape[1] * 4, transcendentals=0),
    )(*given)


def _place_kernel(group, kinds, _, *refs):
    pieces, out, sem = refs[:-2], refs[-2], refs[-1]
    me = lax.axis_index("tp")
    chips = group // 2
    chip, core = me // 2, me % 2
    places = [(chip + by) % chips for by in (2, 2, chips - 1, 0, 1)]
    rows = out.shape[0]
    chunk, piece = 2 * min(ref.shape[0] for ref in pieces), pieces[0].shape[1]
    copies = []
    for n, (kind, ref) in enumerate(zip(kinds, pieces)):
        j = kind % 5
        at = rows - chunk + (chunk // 2 if j == 1 else 0)
        whose = core if kind < 5 else 1 - core
        columns = pl.ds(pl.multiple_of((places[j] * 2 + whose) * piece, piece), piece)
        copies.append(pltpu.make_async_copy(ref, out.at[pl.ds(at, ref.shape[0]), columns], sem.at[n]))
    for copy in copies:
        copy.start()
    for copy in copies:
        copy.wait()


def _place(group, y, kinds, pieces):
    hbm, vmem = pl.BlockSpec(memory_space=pl.ANY), pl.BlockSpec(memory_space=pltpu.VMEM)
    return pl.pallas_call(
        functools.partial(_place_kernel, group, kinds),
        out_shape=jax.ShapeDtypeStruct(y.shape, y.dtype),
        in_specs=[hbm] + [vmem] * len(pieces),
        out_specs=hbm,
        scratch_shapes=[pltpu.SemaphoreType.DMA((len(pieces),))],
        input_output_aliases={0: 0},
        compiler_params=pltpu.CompilerParams(vmem_limit_bytes=16 * 2**20),
        cost_estimate=pl.CostEstimate(flops=10**6, bytes_accessed=10**7, transcendentals=0),
    )(y, *pieces)


def _tables(rows, chunk):
    half = HEAD // 2
    rate = float(THETA) ** (-np.arange(half) / half)

    def pairs(place):
        angle = place[:, None] * rate
        cos, sin = np.cos(angle), np.sin(angle)
        return np.concatenate([cos, cos], -1).astype(np.float32), np.concatenate([-sin, sin], -1).astype(np.float32)

    return *pairs(np.arange(chunk)), *pairs(np.arange(0, rows, chunk))


def solution(mesh):
    group = mesh.shape["tp"]

    def step(x, gain, wq, wk, wv, wo):
        rows, depth = x.shape
        wide = wq.shape[1]
        heads, piece = wide // HEAD, depth // group
        chunk = ROWS
        chunks, half = rows // chunk, chunk // 2
        kb = _fit(depth, BLOCK)
        blocks = depth // kb
        tables = _tables(rows, chunk)
        vmem, hbm = pl.BlockSpec(memory_space=pltpu.VMEM), pl.BlockSpec(memory_space=pl.ANY)
        dma = lambda *shape: pltpu.SemaphoreType.DMA(shape)
        early, done = pl.pallas_call(
            functools.partial(_kernel, group),
            out_shape=[jax.ShapeDtypeStruct((rows, depth), BF16), jax.ShapeDtypeStruct((chunk, piece), BF16)],
            in_specs=[hbm, vmem, hbm, hbm, hbm, hbm, vmem, vmem, vmem, vmem],
            out_specs=[hbm, hbm],
            scratch_shapes=[
                pltpu.VMEM((chunk, depth), BF16),
                pltpu.VMEM((blocks, chunk, kb), BF16),
                pltpu.VMEM((SLOTS, max(kb, wide), max(3 * wide, 2 * piece)), BF16),
                pltpu.VMEM((chunk, 3 * wide), F32),
                pltpu.VMEM((heads, chunk, HEAD), BF16),
                pltpu.VMEM((heads, rows, HEAD), BF16),
                pltpu.VMEM((heads, HEAD + ONES, rows), BF16),
                pltpu.VMEM((heads, chunk), F32),
                pltpu.VMEM((heads, HEAD + ONES, chunk), F32),
                pltpu.VMEM((chunk, wide), BF16),
                pltpu.VMEM((2, group // 2, chunk, piece), F32),
                pltpu.VMEM((group // 2, chunk, piece), BF16),
                pltpu.VMEM((2, group // 2, chunk, piece), BF16),
                pltpu.VMEM((2, half, piece), BF16),
                pltpu.VMEM((2, 2, half, piece), BF16),
                pltpu.VMEM((2, chunk, piece), BF16),
                pltpu.VMEM((2, 2, chunk, piece), BF16),
                pltpu.VMEM((chunk, piece), BF16),
                pltpu.VMEM((2, chunk, piece), BF16),
                pltpu.VMEM((1, depth), F32),
                dma(SLOTS, 3), dma(X_PARTS), dma(2),
                dma(group // 2), dma(2, group // 2),
                dma(2), dma(2, 2),
                dma(2, 2), dma(2, 2, 2),
                dma(2, 2), dma(2, 2, 2),
                dma(2), dma(2, 2),
                dma(group // 2), dma(2, group // 2),
                pltpu.SemaphoreType.DMA,
            ],
            compiler_params=pltpu.CompilerParams(collective_id=0, has_side_effects=True, vmem_limit_bytes=62 * 2**20),
        )(x, gain, wq, wk, wv, wo, *tables)

        right = [(i, (i + 2) % group) for i in range(group)]
        left = [(i, (i - 2) % group) for i in range(group)]
        other = [(i, i + 1 - 2 * (i % 2)) for i in range(group)]
        send = lambda t, to: lax.ppermute(t, "tp", to)
        from_left, from_right, theirs = send(done, right), send(done, left), send(done, other)
        each = chunk // 4
        count = (chunks - 1) * 4
        y = _copy_rows(early, 0, min(SPLIT, count - 1), each)
        y, from_left, from_right = lax.optimization_barrier((y, from_left, from_right))
        opp_a, opp_b = send(from_left[:half], right), send(from_right[half:], left)
        sides = send(from_left, other), send(from_right, other)
        y = _copy_rows(early, min(SPLIT, count - 1), count - min(SPLIT, count - 1), each, y)
        y, opp_a, opp_b = lax.optimization_barrier((y, opp_a, opp_b))
        given = send(opp_a, other), send(opp_b, other)
        y = _place(group, y, (0, 1, 2, 3, 4, 7, 8, 9), (opp_a, opp_b, from_left, done, from_right, sides[0], theirs, sides[1]))
        return _place(group, y, (5, 6), given)

    tokens, columns = P("dp", None), P(None, "tp")
    return jax.shard_map(
        step,
        mesh=mesh,
        in_specs=(tokens, P(None), columns, columns, columns, P("tp", None)),
        out_specs=tokens,
        check_vma=False,
    )
```
